512 devices in a mesh: parts: 2 (over y), seq: 256 (over x, z, core).
Axes of the slice: x: 8, y: 2, z: 16, core: 2. Of those that a mesh axis runs over, the one named last changes fastest.
The devices are a block of a 8x8x16 slice.
Arguments:
- queries: bfloat16 [8, 8192], P('parts', 'seq'), parts along dimension 0
- new_kv: bfloat16 [8, 2048], P('parts', 'seq'), parts along dimension 0, may hold values from -6 to 6
- keys: bfloat16 [1024, 512, 1024], P(('parts', 'seq')), parts along dimension 0, may hold values from -6 to 6
- values: bfloat16 [1024, 512, 1024], P(('parts', 'seq')), parts along dimension 0, may hold values from -6 to 6
- slot_request: int32 [1024], P(('parts', 'seq')), parts along dimension 0, may hold values from 0 to 3, as said below
- slot_length: int32 [1024], P(('parts', 'seq')), parts along dimension 0, may hold values from 1 to 512
Outputs:
- attended: bfloat16 [8, 8192], P('parts'), parts along dimension 0
The draws below stay inside these ranges and needn't reach their ends.
There are 2 independent parts, one for each index of `parts`. The reference program is written for one: setup_inputs(seed, part) draws one part's arguments, and reference() takes and returns one part's arrays. A program takes and returns all parts, laid end to end along the dimension named above; each array names one. Nothing has to cross between parts.
Inputs may be any that keep to these rules, and one draw needn't show every extreme that they name: `slot_request`: every request number 0 to 3 owns at least one block.
All inputs are finite; a program needn't handle non-finite values.
Results may differ from the reference program's by a relative error of at most 0.0055.
Values may be sent and summed in bfloat16 or wider, within the bound.
A program may use at most 128 MiB of HBM per device.

```python
import jax
import jax.numpy as jnp
from jax import lax

H = 64
KVH = 8
DH = 128
BLOCK = 512
REQ = 4
BLOCKS = 512


def draw_queries(key, part):
    return (1.5 * jax.random.normal(jax.random.fold_in(key, 13), (REQ, H * DH), jnp.float32)).astype(jnp.bfloat16)


def draw_slot_request(key, part):
    first = jax.random.randint(jax.random.fold_in(key, 21), (BLOCKS,), 0, REQ)
    second = jax.random.randint(jax.random.fold_in(key, 22), (BLOCKS,), 0, REQ)
    owners = first * second // REQ
    owners = owners.at[:REQ].set(jnp.arange(REQ, dtype=jnp.int32))
    order = jax.random.permutation(jax.random.fold_in(key, 23), BLOCKS)
    return owners[order].astype(jnp.int32)


def draw_slot_length(key, part):
    choose = jax.random.randint(jax.random.fold_in(key, 31), (BLOCKS,), 0, 3)
    short = jax.random.randint(jax.random.fold_in(key, 32), (BLOCKS,), 1, BLOCK + 1)
    filled = jnp.where(choose == 0, short, BLOCK)
    return filled.at[0].set(BLOCK).astype(jnp.int32)


def shard_levels(rng, extent, cuts, smallest, top_value):
    loudness = 1.0
    for dim, parts in cuts:
        heights = jax.random.uniform(jax.random.fold_in(jax.random.fold_in(rng, 6), dim), (parts,), jnp.float32, smallest / len(cuts), top_value / len(cuts))
        loudness = loudness * jnp.repeat(jnp.exp(heights), extent[dim] // parts).reshape((-1,) + (1,) * (len(extent) - 1 - dim))
    return loudness


def bell_draw(rng, dims, width, most, split=(), held_as=jnp.bfloat16):
    level = shard_levels(rng, dims, split, -0.22, 0.18) if split else 1.0
    array = jax.random.normal(rng, dims, jnp.float32) * width * level
    return jnp.minimum(jnp.maximum(array, -most), most).astype(held_as)


def setup_inputs(seed: int = 0, part: int = 0) -> dict:
    key_list = jax.random.split(jax.random.key(seed), 7)
    part_splits = jax.random.split(jax.random.fold_in(key_list[6], part), 7)
    queries = draw_queries(jax.random.fold_in(jax.random.fold_in(key_list[6], part), 71), part)
    new_kv = bell_draw(part_splits[1], (REQ, 2 * KVH * DH), 1.0, 6.0, ((1, 256),))
    keys = bell_draw(part_splits[2], (BLOCKS, BLOCK, KVH * DH), 1.0, 6.0, ((0, 256),))
    values = bell_draw(part_splits[3], (BLOCKS, BLOCK, KVH * DH), 1.0, 6.0, ((0, 256),))
    slot_request = draw_slot_request(jax.random.fold_in(jax.random.fold_in(key_list[6], part), 71), part)
    slot_length = draw_slot_length(jax.random.fold_in(jax.random.fold_in(key_list[6], part), 71), part)
    return dict(queries=queries, new_kv=new_kv, keys=keys, values=values, slot_request=slot_request, slot_length=slot_length)


very_negative = -1e30


def reference(queries, new_kv, keys, values, slot_request, slot_length):
    requests = queries.shape[0]
    group_size = H // KVH
    score_scale = DH ** -0.5
    query_heads = queries.astype(jnp.float32).reshape(requests, KVH, group_size, DH)
    new_pair = new_kv.astype(jnp.float32).reshape(requests, 2, KVH, DH)
    new_score = jnp.einsum("rkgd,rkd->rkg", query_heads, new_pair[:, 0]) * score_scale
    block_count = keys.shape[0]
    key_tiles = keys.reshape(block_count, BLOCK, KVH, DH)
    value_tiles = values.reshape(block_count, BLOCK, KVH, DH)
    positions = jnp.arange(BLOCK, dtype=jnp.int32)

    def block_scores(key_block, request, length):
        picked = query_heads[request]
        scores = jnp.einsum("kgd,tkd->kgt", picked, key_block.astype(jnp.float32)) * score_scale
        inside = positions < length
        return jnp.where(inside[None, None, :], scores, very_negative)

    def first_pass(items):
        key_block, request, length = items
        return jnp.max(block_scores(key_block, request, length), axis=-1)

    block_top = lax.map(first_pass, (key_tiles, slot_request, slot_length))
    owner = slot_request[:, None] == jnp.arange(requests, dtype=jnp.int32)[None, :]
    request_top = jnp.max(jnp.where(owner[:, :, None, None], block_top[:, None], very_negative), axis=0)
    request_top = jnp.maximum(request_top, new_score)

    def second_pass(items):
        key_block, value_block, request, length = items
        scores = block_scores(key_block, request, length)
        weights = jnp.exp(scores - request_top[request][..., None])
        total = jnp.sum(weights, axis=-1)
        rounded = weights.astype(jnp.bfloat16).astype(jnp.float32)
        numer = jnp.einsum("kgt,tkd->kgd", rounded, value_block.astype(jnp.float32))
        return total, numer

    block_sum, block_out = lax.map(second_pass, (key_tiles, value_tiles, slot_request, slot_length))
    owner_float = owner.astype(jnp.float32)
    total = jnp.einsum("br,bkg->rkg", owner_float, block_sum, precision=lax.Precision.HIGHEST)
    numer = jnp.einsum("br,bkgd->rkgd", owner_float, block_out, precision=lax.Precision.HIGHEST)
    new_weight = jnp.exp(new_score - request_top)
    total = total + new_weight
    rounded_new = new_weight.astype(jnp.bfloat16).astype(jnp.float32)
    numer = numer + rounded_new[..., None] * new_pair[:, 1][:, :, None, :]
    attended = numer / total[..., None]
    return attended.reshape(requests, H * DH).astype(jnp.bfloat16)
```

```python
import functools

import jax
import jax.numpy as jnp
from jax import lax
from jax.experimental import pallas as pl
from jax.experimental.pallas import tpu as pltpu
from jax.sharding import Mesh
from jax.sharding import PartitionSpec as P

H = 64
KVH = 8
DH = 128
G = H // KVH
LANES = 128
NX, NZ, NC = 8, 16, 2
AX, AZ, AC = "seq_0", "seq_1", "seq_2"
SEQ = (AX, AZ, AC)
PARTS_SEQ = ("parts", AX, AZ, AC)
NEG = -1e30
MESH = pl.DeviceIdType.MESH
F32, BF16 = jnp.float32, jnp.bfloat16
FAR_X = (4, 3, 5, 2, 6, 1, 7)
FAR_Z = (8, 7, 9, 6, 10, 5, 11, 4, 12, 3, 13, 2, 14, 1, 15)


def iota(shape, dim):
    return lax.broadcasted_iota(jnp.int32, shape, dim)


def at(x, z, c):
    return {AX: x, AZ: z, AC: c}


def wait_for(ref, sem):
    pltpu.make_async_copy(ref, ref, sem).wait()


def kernel(
    req_ref, len_ref, q_ref, kv_ref, k_hbm, v_hbm, out_ref,
    kbuf, vbuf, buf1, g2, kv2, qscr, so, sml, ro, rml, ao, aml,
    load_sem, send_sem, recv_sem, z_sem,
):
    x, z, c = lax.axis_index(AX), lax.axis_index(AZ), lax.axis_index(AC)
    requests, width = q_ref.shape
    new_width = kv_ref.shape[1]
    slots, block = k_hbm.shape[0], k_hbm.shape[1]
    xc = NX * NC
    zh, zl = z // 2, z % 2
    mine_d = zl * NC + c
    mine = x * 4 + mine_d
    scale = DH**-0.5

    barrier = pltpu.get_barrier_semaphore()
    for dx in range(NX):
        for dc in range(NC):
            if dx or dc:
                pl.semaphore_signal(
                    barrier, 1, device_id=at((x + dx) % NX, z, (c + dc) % NC), device_id_type=MESH
                )
    near = (1, 2, 3, 4, NZ - 4, NZ - 3, NZ - 2, NZ - 1)
    for dz in near:
        pl.semaphore_signal(barrier, 1, device_id=at(x, (z + dz) % NZ, c), device_id_type=MESH)

    loads = []
    for s in range(slots):
        loads.append(pltpu.make_async_copy(k_hbm.at[s], kbuf.at[s], load_sem.at[s]))
    for s in range(slots):
        loads.append(pltpu.make_async_copy(v_hbm.at[s], vbuf.at[s], load_sem.at[slots + s]))
    for load in loads:
        load.start()

    def as_row(ref, n):
        spread = (iota((n, LANES), 0) == iota((n, LANES), 1) % n).astype(BF16)
        wide = jnp.dot(ref[...], spread, preferred_element_type=F32)
        keep = iota((requests, LANES), 0) == iota((requests, LANES), 1) // n
        return jnp.sum(jnp.where(keep, wide, 0.0), axis=0, keepdims=True)

    row1 = c * NX + x
    buf1[pl.ds(row1, 1), :, 0:LANES] = as_row(q_ref, width)[None]
    buf1[pl.ds(row1, 1), :, LANES : 2 * LANES] = as_row(kv_ref, new_width)[None]

    req = [req_ref[s] for s in range(slots)]
    length = [len_ref[s] for s in range(slots)]
    lane512 = iota((LANES, 2 * NC * LANES), 1)
    sub512 = iota((LANES, 2 * NC * LANES), 0)
    place = []
    for zp in range(2):
        m = lane512 % LANES
        want = jnp.where((lane512 // LANES) % 2 == 0, req[0], req[1]) * width + m % width
        piece = zp * NC + lane512 // (2 * LANES)
        place.append(((sub512 == want) & (m // width == piece)).astype(BF16))

    pl.semaphore_wait(barrier, xc - 1 + len(near))
    for there in (at(x, (z + 4) % NZ, c), at(x, (z + NZ - 4) % NZ, c), at(x, 2 * zh + 1 - zl, c)):
        pl.semaphore_signal(z_sem, 1, device_id=there, device_id_type=MESH)

    def send(src, dst, phase, there):
        pltpu.make_async_remote_copy(
            src_ref=src,
            dst_ref=dst,
            send_sem=send_sem.at[phase],
            recv_sem=recv_sem.at[phase],
            device_id=there,
            device_id_type=MESH,
        ).start()

    for dx in FAR_X + (0,):
        for dc in range(NC):
            if dx or dc:
                send(buf1.at[row1], buf1.at[row1], 0, at((x + dx) % NX, z, (c + dc) % NC))
    wait_for(buf1.at[pl.ds(0, xc - 1)], recv_sem.at[0])
    rows = buf1[:, 0, :]
    g2[pl.ds(z, 1)] = rows[:, 0:LANES].astype(BF16)[None]
    kv2[pl.ds(z, 1)] = rows[:, LANES : 2 * LANES].astype(BF16)[None]

    pl.semaphore_wait(z_sem, 3)
    for dz in FAR_Z:
        send(g2.at[z], g2.at[z], 1, at(x, (z + dz) % NZ, c))
    for dz in FAR_Z:
        send(kv2.at[z], kv2.at[z], 2, at(x, (z + dz) % NZ, c))
    for load in loads:
        load.wait()
    wait_for(g2.at[pl.ds(0, NZ - 1)], recv_sem.at[1])

    picked = [None, None]
    for zp in range(2):
        lhs = jnp.concatenate([g2[2 * i + zp] for i in range(G)], axis=0)
        placed = jnp.dot(lhs, place[zp], preferred_element_type=F32).reshape(G, xc, 2 * NC * LANES)
        for s in range(slots):
            for cc in range(NC):
                at_lane = (cc * 2 + s) * LANES
                part = placed[:, cc * NX : (cc + 1) * NX, at_lane : at_lane + LANES]
                picked[s] = part if picked[s] is None else picked[s] + part
    for s in range(slots):
        qscr[s] = picked[s]

    lane = iota((G, LANES), 1)
    lane_s, lane_hh, lane_r = (lane // 8) % 2, (lane // 4) % 2, lane % 4
    inside = [iota((G, block), 1) < length[s] for s in range(slots)]
    order = FAR_X + (0,)
    weights, vals = {}, {}
    for n, dx in enumerate(order):
        k = (x + dx) % NX
        cols = pl.ds(pl.multiple_of(k * DH, DH), DH)
        tops, sums = [], []
        for s in range(slots):
            qk = qscr[s, :, k, :].astype(BF16)
            sc = lax.dot_general(
                qk, kbuf[s, :, cols], (((1,), (1,)), ((), ())), preferred_element_type=F32
            )
            sc = jnp.where(inside[s], sc * scale, NEG)
            top = jnp.max(sc, axis=1, keepdims=True)
            w = jnp.exp(sc - top)
            tops.append(top)
            sums.append(jnp.sum(w, axis=1, keepdims=True))
            weights[n, s] = w.astype(BF16)
        of_slot = [
            jnp.where(
                lane < 64,
                jnp.where(lane_r == req[s], tops[s], NEG),
                jnp.where(lane_r == req[s], sums[s], 0.0),
            )
            for s in range(slots)
        ]
        vals[n] = jnp.where(lane_s == 0, of_slot[0], of_slot[1])
    for n, dx in enumerate(order):
        k = (x + dx) % NX
        cols = pl.ds(pl.multiple_of(k * DH, DH), DH)
        for d in range(4):
            sml[n, d] = jnp.where(
                lane_hh[0:1] == 0, vals[n][2 * d : 2 * d + 1], vals[n][2 * d + 1 : 2 * d + 2]
            )
        for s in range(slots):
            o = jnp.dot(weights[n, s], vbuf[s, :, cols], preferred_element_type=F32)
            for d in range(4):
                so[n, d, 2 * s : 2 * s + 2, :] = o[2 * d : 2 * d + 2]
        for dd in range(4):
            if dx or dd:
                d = dd if dx else (mine_d + dd) % 4
                there = at(k, 2 * zh + d // NC, d % NC)
                send(sml.at[n, d], rml.at[mine], 4, there)
                send(so.at[n, d], ro.at[mine], 3, there)
    last = len(order) - 1
    ro[pl.ds(mine, 1)] = so[last, pl.ds(mine_d, 1)]
    rml[pl.ds(mine, 1)] = sml[last, pl.ds(mine_d, 1)]

    wait_for(kv2.at[pl.ds(0, NZ - 1)], recv_sem.at[2])
    total_rows = NZ * xc
    u, col = iota((2 * xc, total_rows), 0), iota((2 * xc, total_rows), 1)
    source = (
        ((x % 2) * (NZ // 2) + (u % xc) // NC) * xc + (u % NC) * NX + x // 2 + (NX // 2) * (u // xc)
    )
    pick = (col == source).astype(BF16)
    new = jnp.dot(pick, kv2[...].reshape(total_rows, LANES), preferred_element_type=F32)
    wide_l, wide_m = iota((LANES, requests * LANES), 0), iota((LANES, requests * LANES), 1)
    wide_r, wide_m = wide_m // LANES, wide_m % LANES
    to_new = (wide_l == wide_r * new_width + wide_m % new_width).astype(BF16)
    to_q = (wide_l == wide_r * width + wide_m % width).astype(BF16)
    new = jnp.dot(new.astype(BF16), to_new, preferred_element_type=F32)
    keep = (iota(new.shape, 1) % LANES) // new_width == iota(new.shape, 0) % xc
    new = jnp.where(keep, new, 0.0)

    def by_request(flat):
        return [flat[:, r * LANES : (r + 1) * LANES] for r in range(requests)]

    new_k = by_request(jnp.sum(new[0:xc], axis=0, keepdims=True))
    new_v = by_request(jnp.sum(new[xc : 2 * xc], axis=0, keepdims=True))
    u, col = iota((8, total_rows), 0), iota((8, total_rows), 1)
    member = 2 * mine_d + u // 4
    source = (2 * member + (u % 4) // NC) * xc + (u % NC) * NX + x
    pick = (col == source).astype(BF16)
    own_q = jnp.dot(pick, g2[...].reshape(total_rows, LANES), preferred_element_type=F32)
    own_q = jnp.dot(own_q.astype(BF16), to_q, preferred_element_type=F32)
    keep = (iota(own_q.shape, 1) % LANES) // width == iota(own_q.shape, 0) % 4
    own_q = jnp.where(keep, own_q, 0.0)
    q_rows = by_request(jnp.sum(own_q[0:4], axis=0, keepdims=True)) + by_request(
        jnp.sum(own_q[4:8], axis=0, keepdims=True)
    )
    q_rows = jnp.concatenate(q_rows, axis=0)
    k_rows = jnp.concatenate(new_k + new_k, axis=0)
    v_rows = jnp.concatenate(new_v + new_v, axis=0)
    new_score = jnp.sum(q_rows * k_rows, axis=1, keepdims=True) * scale

    group = 4 * NX
    wait_for(rml.at[pl.ds(0, group - 1)], recv_sem.at[4])
    ml = rml[:, 0, :]
    top = jnp.max(ml, axis=0, keepdims=True)
    top = jnp.maximum(top, pltpu.roll(top, 8, 1))
    w = jnp.exp(ml - top)
    total = jnp.sum(w * pltpu.roll(ml, 64, 1), axis=0, keepdims=True)
    total = total + pltpu.roll(total, 8, 1)
    lane1 = iota((1, LANES), 1)
    aml[pl.ds(zh, 1)] = jnp.where(lane1 < 64, top, pltpu.roll(total, 64, 1))[None]
    wait_for(ro.at[pl.ds(0, group - 1)], recv_sem.at[3])
    merged = []
    for hh in range(2):
        planes = [ro[:, s * 2 + hh, :] for s in range(slots)]
        for r in range(requests):
            acc = None
            for s in range(slots):
                i = 16 + s * 8 + hh * 4 + r
                part = w[:, i : i + 1] * planes[s]
                acc = part if acc is None else acc + part
            merged.append(jnp.sum(acc, axis=0, keepdims=True))
    ao[pl.ds(zh, 1)] = jnp.concatenate(merged, axis=0)[None]

    for dz in FAR_X:
        there = at(x, 2 * ((zh + dz) % NX) + zl, c)
        send(aml.at[zh], aml.at[zh], 6, there)
        send(ao.at[zh], ao.at[zh], 5, there)
    pairs = NZ // 2
    wait_for(aml.at[pl.ds(0, pairs - 1)], recv_sem.at[6])
    sub = iota((8, LANES), 0)
    lane8 = iota((8, LANES), 1)
    m_at, l_at = lane8 == 16 + sub, lane8 == 80 + sub
    ms = [jnp.sum(jnp.where(m_at, aml[i], 0.0), axis=1, keepdims=True) for i in range(pairs)]
    ls = [jnp.sum(jnp.where(l_at, aml[i], 0.0), axis=1, keepdims=True) for i in range(pairs)]
    peak = functools.reduce(jnp.maximum, ms, new_score)
    new_w = jnp.exp(new_score - peak)
    factors = [jnp.exp(m - peak) for m in ms]
    denom = new_w
    for i in range(pairs):
        denom = denom + factors[i] * ls[i]
    wait_for(ao.at[pl.ds(0, pairs - 1)], recv_sem.at[5])
    numer = new_w * v_rows
    for i in range(pairs):
        numer = numer + factors[i] * ao[i]
    final = (numer / denom).astype(BF16)

    base = pl.multiple_of(mine * 2 * DH, 2 * DH)
    out_ref[:, pl.ds(base, DH)] = final[0:4]
    out_ref[:, pl.ds(pl.multiple_of(base + DH, DH), DH)] = final[4:8]
    here = out_ref.at[:, pl.ds(base, 2 * DH)]
    for dx in FAR_X + (0,):
        for dd in range(4):
            if dx or dd:
                d = (mine_d + dd) % 4
                send(here, here, 7, at((x + dx) % NX, 2 * zh + d // NC, d % NC))
    wait_for(out_ref.at[:, pl.ds(0, (group - 1) * 2 * DH)], recv_sem.at[7])

    wait_for(buf1.at[pl.ds(0, xc - 1)], send_sem.at[0])
    wait_for(g2.at[pl.ds(0, NZ - 1)], send_sem.at[1])
    wait_for(kv2.at[pl.ds(0, NZ - 1)], send_sem.at[2])
    wait_for(ro.at[pl.ds(0, group - 1)], send_sem.at[3])
    wait_for(rml.at[pl.ds(0, group - 1)], send_sem.at[4])
    wait_for(ao.at[pl.ds(0, pairs - 1)], send_sem.at[5])
    wait_for(aml.at[pl.ds(0, pairs - 1)], send_sem.at[6])
    wait_for(out_ref.at[:, pl.ds(0, (group - 1) * 2 * DH)], send_sem.at[7])


def shards(queries, new_kv, keys, values, slot_request, slot_length):
    slots, block, columns = keys.shape
    requests = queries.shape[0]
    xc, group = NX * NC, 4 * NX
    smem = pl.BlockSpec(memory_space=pltpu.SMEM)
    vmem = pl.BlockSpec(memory_space=pltpu.VMEM)
    hbm = pl.BlockSpec(memory_space=pl.ANY)
    return pl.pallas_call(
        kernel,
        out_shape=jax.ShapeDtypeStruct((requests, H * DH), BF16),
        in_specs=[smem, smem, vmem, vmem, hbm, hbm],
        out_specs=vmem,
        scratch_shapes=[
            pltpu.VMEM((slots, block, columns), BF16),
            pltpu.VMEM((slots, block, columns), BF16),
            pltpu.VMEM((xc, 1, 2 * LANES), F32),
            pltpu.VMEM((NZ, xc, LANES), BF16),
            pltpu.VMEM((NZ, xc, LANES), BF16),
            pltpu.VMEM((slots, G, KVH, DH), F32),
            pltpu.VMEM((KVH, 4, 4, DH), F32),
            pltpu.VMEM((KVH, 4, 1, LANES), F32),
            pltpu.VMEM((group, 4, DH), F32),
            pltpu.VMEM((group, 1, LANES), F32),
            pltpu.VMEM((NZ // 2, 8, DH), F32),
            pltpu.VMEM((NZ // 2, 1, LANES), F32),
            pltpu.SemaphoreType.DMA((2 * slots,)),
            pltpu.SemaphoreType.DMA((8,)),
            pltpu.SemaphoreType.DMA((8,)),
            pltpu.SemaphoreType.REGULAR,
        ],
        compiler_params=pltpu.CompilerParams(collective_id=0, has_side_effects=True),
        cost_estimate=pl.CostEstimate(
            flops=4 * slots * block * H * DH,
            bytes_accessed=4 * slots * block * columns,
            transcendentals=slots * block * H,
        ),
        name="decode",
    )(slot_request, slot_length, queries, new_kv, keys, values)


def solution(mesh):
    torus = Mesh(mesh.devices.reshape(mesh.shape["parts"], NX, NZ, NC), ("parts",) + SEQ)
    placed = (
        P("parts", SEQ),
        P("parts", SEQ),
        P(PARTS_SEQ, None, None),
        P(PARTS_SEQ, None, None),
        P(PARTS_SEQ),
        P(PARTS_SEQ),
    )
    return jax.shard_map(
        shards, mesh=torus, in_specs=placed, out_specs=P("parts", None), check_vma=False
    )
```

```python
import functools

import jax
import jax.numpy as jnp
from jax import lax
from jax.experimental import pallas as pl
from jax.experimental.pallas import tpu as pltpu
from jax.sharding import Mesh
from jax.sharding import PartitionSpec as P

H = 64
KVH = 8
DH = 128
G = H // KVH
LANES = 128
NX, NZ, NC = 8, 16, 2
AX, AZ, AC = "seq_0", "seq_1", "seq_2"
SEQ = (AX, AZ, AC)
PARTS_SEQ = ("parts", AX, AZ, AC)
NEG = -1e30
MESH = pl.DeviceIdType.MESH
F32, BF16 = jnp.float32, jnp.bfloat16
FAR_X = (4, 3, 5, 2, 6, 1, 7)
FAR_Z = (8, 7, 9, 6, 10, 5, 11, 4, 12, 3, 13, 2, 14, 1, 15)


def iota(shape, dim):
    return lax.broadcasted_iota(jnp.int32, shape, dim)


def at(x, z, c):
    return {AX: x, AZ: z, AC: c}


def wait_for(ref, sem):
    pltpu.make_async_copy(ref, ref, sem).wait()


def kernel(
    req_hbm, len_hbm, q_hbm, kv_hbm, k_hbm, v_hbm, out_ref,
    req_ref, len_ref, q_ref, kv_ref, kbuf, vbuf, above, below, g2, kv2, qscr, so, sml, ro, rml, ao, aml,
    load_sem, small_sem, send_sem, recv_sem, row_sem, x_sem, top_sem, pair_sem,
):
    x, z, c = lax.axis_index(AX), lax.axis_index(AZ), lax.axis_index(AC)
    requests, width = q_ref.shape
    new_width = kv_ref.shape[1]
    slots, block = k_hbm.shape[0], k_hbm.shape[1]
    xc = NX * NC
    zh, zl = z // 2, z % 2
    mine_d = c * 2 + zl
    mine = x * 4 + mine_d
    scale = DH**-0.5

    top_z = NZ - 1
    small = [
        pltpu.make_async_copy(src, dst, small_sem.at[i])
        for i, (src, dst) in enumerate(
            ((q_hbm, q_ref), (kv_hbm, kv_ref), (req_hbm, req_ref), (len_hbm, len_ref))
        )
    ]
    small[0].start()
    small[1].start()
    barrier = pltpu.get_barrier_semaphore()
    others = [(dx, dc) for dx in FAR_X + (0,) for dc in range(NC) if dx or dc]

    def on_z(z_there):
        return at(x, z_there % NZ, c)

    def plane_mate(dx, dc, z_there):
        return at((x + dx) % NX, z_there % NZ, (c + dc) % NC)

    @pl.when((z > 0) & (z < top_z))
    def _():
        pl.semaphore_signal(barrier, 1, device_id=on_z(NZ), device_id_type=MESH)

    @pl.when(z == 1)
    def _():
        pl.semaphore_signal(barrier, 1, device_id=at(x, z, 1 - c), device_id_type=MESH)

    @pl.when(z == 0)
    def _():
        for dx, dc in others + [(0, 0)]:
            there = plane_mate(dx, dc, top_z)
            pl.semaphore_signal(barrier, 1, device_id=there, device_id_type=MESH)

    for i in FAR_Z:

        @pl.when((z > 0) & (z + i < NZ))
        def _(i=i):
            pl.semaphore_signal(barrier, 1, device_id=on_z(z + i), device_id_type=MESH)

    @pl.when((z > 0) & (z + 2 < NZ))
    def _():
        for dx, dc in others:
            there = plane_mate(dx, dc, z + 2)
            pl.semaphore_signal(barrier, 1, device_id=there, device_id_type=MESH)

    loads = []
    for s in range(slots):
        loads.append(pltpu.make_async_copy(k_hbm.at[s], kbuf.at[s], load_sem.at[s]))
    for s in range(slots):
        loads.append(pltpu.make_async_copy(v_hbm.at[s], vbuf.at[s], load_sem.at[slots + s]))
    for load in small[2:] + loads:
        load.start()

    def as_row(ref, n):
        spread = (iota((n, LANES), 0) == iota((n, LANES), 1) % n).astype(BF16)
        wide = jnp.dot(ref[...], spread, preferred_element_type=F32)
        keep = iota((requests, LANES), 0) == iota((requests, LANES), 1) // n
        return jnp.sum(jnp.where(keep, wide, 0.0), axis=0, keepdims=True)

    place_z = zl * G + zh
    small[0].wait()
    small[1].wait()
    own = jnp.concatenate([as_row(q_ref, width), as_row(kv_ref, new_width)], axis=1)[None]
    above[pl.ds(place_z, 1)] = own

    def send(src, dst, phase, there, recv=None):
        pltpu.make_async_remote_copy(
            src_ref=src,
            dst_ref=dst,
            send_sem=send_sem.at[phase],
            recv_sem=recv_sem.at[phase] if recv is None else recv,
            device_id=there,
            device_id_type=MESH,
        ).start()

    greeted = z - 1 + jnp.where(z > 2, xc - 1, 0)
    greeted = greeted + jnp.where(z == top_z, xc, 0)
    pl.semaphore_wait(barrier, jnp.where(z == 0, NZ - 2, jnp.where(z == 1, 1, greeted)))

    row = above.at[place_z]

    def greeter(i):
        if i == 1:
            return z > 1
        return (z > i) | (z == 0) if i < top_z else (z == 0) | (z == top_z)

    for i in FAR_Z:

        @pl.when(greeter(i))
        def _(i=i):
            send(row, row, 8 + i, on_z(z + NZ - i), row_sem.at[z])

    @pl.when(z > 2)
    def _():
        pl.semaphore_signal(x_sem, 1, device_id=on_z(z + NZ - 2), device_id_type=MESH)

    @pl.when(z == top_z)
    def _():
        pl.semaphore_signal(x_sem, 1, device_id=on_z(NZ), device_id_type=MESH)

    @pl.when(z >= top_z - 1)
    def _():
        for dx, dc in others + [(0, 0)]:
            there = plane_mate(dx, dc, z + NZ - 2)
            pl.semaphore_signal(top_sem, 1, device_id=there, device_id_type=MESH)

    @pl.when((z == 1) | (z == 2))
    def _():
        below[...] = jnp.zeros_like(below)

    @pl.when((z > 0) & (z < top_z))
    def _():
        wait_for(row, row_sem.at[z + 1])
        send(row, row, 8 + NZ, on_z(z + 1), row_sem.at[z])

    @pl.when(z > 2)
    def _():
        wait_for(below, recv_sem.at[0])

    @pl.when(z > 1)
    def _():
        wait_for(row, row_sem.at[z - 1])
        below_z = (1 - zl) * G + (z - 1) // 2
        below[pl.ds(below_z, 1)] = above[pl.ds(below_z, 1)]

    @pl.when(z > 0)
    def _():
        below[pl.ds(place_z, 1)] = own

    @pl.when(z == top_z - 1)
    def _():
        wait_for(row, row_sem.at[0])
        send(below, below, 8, on_z(NZ), recv_sem.at[0])

    @pl.when((z > 0) & (z < top_z - 1))
    def _():
        wait_for(row, row_sem.at[z + 2])
        send(below, below, 0, on_z(z + 2), recv_sem.at[0])

    @pl.when(z == 0)
    def _():
        wait_for(row, row_sem.at[top_z])
        send(row, row, 9, on_z(top_z), row_sem.at[0])
        wait_for(below, recv_sem.at[0])

    small[2].wait()
    small[3].wait()
    req = [req_ref[s] for s in range(slots)]
    length = [len_ref[s] for s in range(slots)]
    lane512 = iota((LANES, 2 * NC * LANES), 1)
    sub512 = iota((LANES, 2 * NC * LANES), 0)
    place = []
    for cc in range(NC):
        m = lane512 % LANES
        want = jnp.where((lane512 // LANES) % 2 == 0, req[0], req[1]) * width + m % width
        piece = (lane512 // (2 * LANES)) * NC + cc
        place.append(((sub512 == want) & (m // width == piece)).astype(BF16))

    for i in range(3, NZ):

        @pl.when((z > 0) & (z + i < NZ))
        def _(i=i):
            wait_for(row, row_sem.at[z + i])

    @pl.when((z > 0) & (z != top_z - 1))
    def _():
        wait_for(row, row_sem.at[0])

    @pl.when((z >= top_z - 3) & (z < top_z - 1))
    def _():
        pl.semaphore_wait(top_sem, xc)
        pl.semaphore_signal(x_sem, 1, device_id=on_z(z + 2), device_id_type=MESH)

    z_of = iota((NZ, 2 * LANES), 0)
    z_of = 2 * (z_of % G) + z_of // G
    from_below = (z_of > 0) & (z_of < jnp.where(z == 0, top_z, z))
    rows = jnp.where(from_below, below[:, 0, :], above[:, 0, :]).astype(BF16)
    row1 = c * NX + x
    g2[pl.ds(row1, 1)] = rows[:, 0:LANES][None]
    kv2[pl.ds(row1, 1)] = rows[:, LANES : 2 * LANES][None]

    pl.semaphore_wait(x_sem, 1)
    for dx, dc in others:
        send(g2.at[row1], g2.at[row1], 1, plane_mate(dx, dc, z))
    for dx, dc in others:
        send(kv2.at[row1], kv2.at[row1], 2, plane_mate(dx, dc, z))
    pl.semaphore_signal(pair_sem, 1, device_id=at(x, 2 * zh + 1 - zl, c), device_id_type=MESH)
    for load in loads:
        load.wait()
    wait_for(g2.at[pl.ds(0, xc - 1)], recv_sem.at[1])

    picked = [None, None]
    for cc in range(NC):
        lhs = g2[cc * NX : (cc + 1) * NX].reshape(NX * NZ, LANES)
        placed = jnp.dot(lhs, place[cc], preferred_element_type=F32).reshape(NX, NZ, 4 * LANES)
        for s in range(slots):
            for zp in range(2):
                at_lane = (zp * 2 + s) * LANES
                part = placed[:, zp * G : (zp + 1) * G, at_lane : at_lane + LANES]
                picked[s] = part if picked[s] is None else picked[s] + part
    for s in range(slots):
        qscr[s] = picked[s].astype(BF16)
    pl.semaphore_wait(pair_sem, 1)

    lane = iota((G, LANES), 1)
    lane_s, lane_hh, lane_r = (lane // 8) % 2, (lane // 4) % 2, lane % 4
    inside = [iota((G, block), 1) < length[s] for s in range(slots)]
    order = FAR_X + (0,)
    weights, vals = {}, {}
    for n, dx in enumerate(order):
        k = (x + dx) % NX
        cols = pl.ds(pl.multiple_of(k * DH, DH), DH)
        tops, sums = [], []
        for s in range(slots):
            qk = qscr[s, k]
            sc = lax.dot_general(
                qk, kbuf[s, :, cols], (((1,), (1,)), ((), ())), preferred_element_type=F32
            )
            sc = jnp.where(inside[s], sc * scale, NEG)
            top = jnp.max(sc, axis=1, keepdims=True)
            w = jnp.exp(sc - top)
            tops.append(top)
            sums.append(jnp.sum(w, axis=1, keepdims=True))
            weights[n, s] = w.astype(BF16)
        of_slot = [
            jnp.where(
                lane < 64,
                jnp.where(lane_r == req[s], tops[s], NEG),
                jnp.where(lane_r == req[s], sums[s], 0.0),
            )
            for s in range(slots)
        ]
        vals[n] = jnp.where(lane_s == 0, of_slot[0], of_slot[1])
    for n, dx in enumerate(order):
        k = (x + dx) % NX
        cols = pl.ds(pl.multiple_of(k * DH, DH), DH)
        for d in range(4):
            sml[n, d] = jnp.where(
                lane_hh[0:1] == 0, vals[n][2 * d : 2 * d + 1], vals[n][2 * d + 1 : 2 * d + 2]
            )
        for s in range(slots):
            o = jnp.dot(weights[n, s], vbuf[s, :, cols], preferred_element_type=F32)
            for d in range(4):
                so[n, d, 2 * s : 2 * s + 2, :] = o[2 * d : 2 * d + 2]
        for dd in range(4):
            if dx or dd:
                d = dd if dx else (mine_d + dd) % 4
                there = at(k, 2 * zh + d % 2, d // 2)
                send(sml.at[n, d], rml.at[mine], 4, there)
                send(so.at[n, d], ro.at[mine], 3, there)
    last = len(order) - 1
    ro[pl.ds(mine, 1)] = so[last, pl.ds(mine_d, 1)]
    rml[pl.ds(mine, 1)] = sml[last, pl.ds(mine_d, 1)]

    wait_for(kv2.at[pl.ds(0, xc - 1)], recv_sem.at[2])
    total_rows = NZ * xc
    u, col = iota((2 * xc, total_rows), 0), iota((2 * xc, total_rows), 1)
    zi = (u % xc) // NC
    from_row = (u % NC) * NX + x // 2 + (NX // 2) * (u // xc)
    source = from_row * NZ + (zi % 2) * G + (x % 2) * (G // 2) + zi // 2
    pick = (col == source).astype(BF16)
    new = jnp.dot(pick, kv2[...].reshape(total_rows, LANES), preferred_element_type=F32)
    wide_l, wide_m = iota((LANES, requests * LANES), 0), iota((LANES, requests * LANES), 1)
    wide_r, wide_m = wide_m // LANES, wide_m % LANES
    to_new = (wide_l == wide_r * new_width + wide_m % new_width).astype(BF16)
    to_q = (wide_l == wide_r * width + wide_m % width).astype(BF16)
    new = jnp.dot(new.astype(BF16), to_new, preferred_element_type=F32)
    keep = (iota(new.shape, 1) % LANES) // new_width == iota(new.shape, 0) % xc
    new = jnp.where(keep, new, 0.0)

    def by_request(flat):
        return [flat[:, r * LANES : (r + 1) * LANES] for r in range(requests)]

    new_k = by_request(jnp.sum(new[0:xc], axis=0, keepdims=True))
    new_v = by_request(jnp.sum(new[xc : 2 * xc], axis=0, keepdims=True))
    u, col = iota((16, total_rows), 0), iota((16, total_rows), 1)
    source = ((u % NC) * NX + x) * NZ + ((u % 4) // NC) * G + 4 * c + u // 4
    pick = (col == source).astype(BF16)
    own_q = jnp.dot(pick, g2[...].reshape(total_rows, LANES), preferred_element_type=F32)
    own_q = jnp.dot(own_q.astype(BF16), to_q, preferred_element_type=F32)
    keep = (iota(own_q.shape, 1) % LANES) // width == iota(own_q.shape, 0) % 4
    own_q = jnp.where(keep, own_q, 0.0)
    k_rows = jnp.concatenate(new_k + new_k, axis=0)
    v_rows = jnp.concatenate(new_v + new_v, axis=0)
    new_score = []
    for half in range(2):
        q_rows = []
        for hh in range(2):
            i = (half * 2 + hh) * 4
            q_rows += by_request(jnp.sum(own_q[i : i + 4], axis=0, keepdims=True))
        q_rows = jnp.concatenate(q_rows, axis=0)
        new_score.append(jnp.sum(q_rows * k_rows, axis=1, keepdims=True) * scale)

    group = 4 * NX
    wait_for(rml.at[pl.ds(0, group - 1)], recv_sem.at[4])
    ml = rml[:, 0, :]
    top = jnp.max(ml, axis=0, keepdims=True)
    top = jnp.maximum(top, pltpu.roll(top, 8, 1))
    w = jnp.exp(ml - top)
    total = jnp.sum(w * pltpu.roll(ml, 64, 1), axis=0, keepdims=True)
    total = total + pltpu.roll(total, 8, 1)
    lane1 = iota((1, LANES), 1)
    aml[pl.ds(z, 1)] = jnp.where(lane1 < 64, top, pltpu.roll(total, 64, 1))[None]
    wait_for(ro.at[pl.ds(0, group - 1)], recv_sem.at[3])
    merged = []
    for hh in range(2):
        planes = [ro[:, s * 2 + hh, :] for s in range(slots)]
        for r in range(requests):
            acc = None
            for s in range(slots):
                i = 16 + s * 8 + hh * 4 + r
                part = w[:, i : i + 1] * planes[s]
                acc = part if acc is None else acc + part
            merged.append(jnp.sum(acc, axis=0, keepdims=True))
    ao[pl.ds(z, 1)] = jnp.concatenate(merged, axis=0)[None]

    for i in range(NZ):

        @pl.when(z != i)
        def _(i=i):
            send(aml.at[z], aml.at[z], 6, on_z(i))
            send(ao.at[z], ao.at[z], 5, on_z(i))

    wait_for(aml.at[pl.ds(0, NZ - 1)], recv_sem.at[6])
    sub = iota((8, LANES), 0)
    lane8 = iota((8, LANES), 1)
    m_at, l_at = lane8 == 16 + sub, lane8 == 80 + sub
    ways = []
    for half in range(2):
        planes = range(half, NZ, 2)
        ms = [jnp.sum(jnp.where(m_at, aml[i], 0.0), axis=1, keepdims=True) for i in planes]
        ls = [jnp.sum(jnp.where(l_at, aml[i], 0.0), axis=1, keepdims=True) for i in planes]
        peak = functools.reduce(jnp.maximum, ms, new_score[half])
        new_w = jnp.exp(new_score[half] - peak)
        factors = [jnp.exp(m - peak) for m in ms]
        denom = new_w
        for factor, part in zip(factors, ls):
            denom = denom + factor * part
        ways.append((new_w, factors, denom))
    wait_for(ao.at[pl.ds(0, NZ - 1)], recv_sem.at[5])
    base = pl.multiple_of((x * NC + c) * 4 * DH, 4 * DH)
    for half in range(2):
        new_w, factors, denom = ways[half]
        numer = new_w * v_rows
        for i, factor in zip(range(half, NZ, 2), factors):
            numer = numer + factor * ao[i]
        final = (numer / denom).astype(BF16)
        for hh in range(2):
            start = pl.multiple_of(base + (half * 2 + hh) * DH, DH)
            out_ref[:, pl.ds(start, DH)] = final[hh * 4 : hh * 4 + 4]

    here = out_ref.at[:, pl.ds(base, 4 * DH)]
    for dx, dc in others:
        send(here, here, 7, plane_mate(dx, dc, z))
    wait_for(out_ref.at[:, pl.ds(0, (xc - 1) * 4 * DH)], recv_sem.at[7])

    for i in range(1, NZ):

        @pl.when(greeter(i) if i > 1 else z != 1)
        def _(i=i):
            wait_for(row, send_sem.at[8 + i])

    @pl.when((z > 0) & (z < top_z))
    def _():
        wait_for(row, send_sem.at[8 + NZ])

    @pl.when((z > 0) & (z < top_z - 1))
    def _():
        wait_for(below, send_sem.at[0])

    @pl.when(z == top_z - 1)
    def _():
        wait_for(below, send_sem.at[8])

    wait_for(g2.at[pl.ds(0, xc - 1)], send_sem.at[1])
    wait_for(kv2.at[pl.ds(0, xc - 1)], send_sem.at[2])
    wait_for(ro.at[pl.ds(0, group - 1)], send_sem.at[3])
    wait_for(rml.at[pl.ds(0, group - 1)], send_sem.at[4])
    wait_for(ao.at[pl.ds(0, NZ - 1)], send_sem.at[5])
    wait_for(aml.at[pl.ds(0, NZ - 1)], send_sem.at[6])
    wait_for(out_ref.at[:, pl.ds(0, (xc - 1) * 4 * DH)], send_sem.at[7])


def shards(queries, new_kv, keys, values, slot_request, slot_length):
    slots, block, columns = keys.shape
    requests = queries.shape[0]
    xc, group = NX * NC, 4 * NX
    vmem = pl.BlockSpec(memory_space=pltpu.VMEM)
    hbm = pl.BlockSpec(memory_space=pl.ANY)
    return pl.pallas_call(
        kernel,
        out_shape=pltpu.VMEM((requests, H * DH), BF16),
        in_specs=[hbm] * 6,
        out_specs=vmem,
        scratch_shapes=[
            pltpu.SMEM(slot_request.shape, jnp.int32),
            pltpu.SMEM(slot_length.shape, jnp.int32),
            pltpu.VMEM(queries.shape, BF16),
            pltpu.VMEM(new_kv.shape, BF16),
            pltpu.VMEM((slots, block, columns), BF16),
            pltpu.VMEM((slots, block, columns), BF16),
            pltpu.VMEM((NZ, 1, 2 * LANES), F32),
            pltpu.VMEM((NZ, 1, 2 * LANES), F32),
            pltpu.VMEM((xc, NZ, LANES), BF16),
            pltpu.VMEM((xc, NZ, LANES), BF16),
            pltpu.VMEM((slots, KVH, G, DH), BF16),
            pltpu.VMEM((KVH, 4, 4, DH), F32),
            pltpu.VMEM((KVH, 4, 1, LANES), F32),
            pltpu.VMEM((group, 4, DH), F32),
            pltpu.VMEM((group, 1, LANES), F32),
            pltpu.VMEM((NZ, 8, DH), F32),
            pltpu.VMEM((NZ, 1, LANES), F32),
            pltpu.SemaphoreType.DMA((2 * slots,)),
            pltpu.SemaphoreType.DMA((4,)),
            pltpu.SemaphoreType.DMA((9 + NZ,)),
            pltpu.SemaphoreType.DMA((8,)),
            pltpu.SemaphoreType.DMA((NZ,)),
            pltpu.SemaphoreType.REGULAR,
            pltpu.SemaphoreType.REGULAR,
            pltpu.SemaphoreType.REGULAR,
        ],
        compiler_params=pltpu.CompilerParams(collective_id=0, has_side_effects=True),
        cost_estimate=pl.CostEstimate(
            flops=4 * slots * block * H * DH,
            bytes_accessed=4 * slots * block * columns,
            transcendentals=slots * block * H,
        ),
        name="decode",
    )(slot_request, slot_length, queries, new_kv, keys, values)


def solution(mesh):
    torus = Mesh(mesh.devices.reshape(mesh.shape["parts"], NX, NZ, NC), ("parts",) + SEQ)
    placed = (
        P("parts", SEQ),
        P("parts", SEQ),
        P(PARTS_SEQ, None, None),
        P(PARTS_SEQ, None, None),
        P(PARTS_SEQ),
        P(PARTS_SEQ),
    )
    return jax.shard_map(
        shards, mesh=torus, in_specs=placed, out_specs=P("parts", None), check_vma=False
    )
```

```python
import functools

import jax
import jax.numpy as jnp
from jax import lax
from jax.experimental import pallas as pl
from jax.experimental.pallas import tpu as pltpu
from jax.sharding import Mesh
from jax.sharding import PartitionSpec as P

H = 64
KVH = 8
DH = 128
G = H // KVH
LANES = 128
NX, NZ, NC = 8, 16, 2
AX, AZ, AC = "seq_0", "seq_1", "seq_2"
SEQ = (AX, AZ, AC)
PARTS_SEQ = ("parts", AX, AZ, AC)
NEG = -1e30
MESH = pl.DeviceIdType.MESH
F32, BF16 = jnp.float32, jnp.bfloat16
FAR_X = (4, 3, 5, 2, 6, 1, 7)
FAR_Z = (8, 7, 9, 6, 10, 5, 11, 4, 12, 3, 13, 2, 14, 1, 15)


def iota(shape, dim):
    return lax.broadcasted_iota(jnp.int32, shape, dim)


def at(x, z, c):
    return {AX: x, AZ: z, AC: c}


def wait_for(ref, sem):
    pltpu.make_async_copy(ref, ref, sem).wait()


def kernel(
    req_hbm, len_hbm, q_hbm, kv_hbm, k_hbm, v_hbm, out_ref,
    req_ref, len_ref, q_ref, kv_ref, kbuf, vbuf, above, below, g2, kv2, qscr, so, sml, ro, rml, ao, aml,
    load_sem, small_sem, send_sem, recv_sem, row_sem, x_sem, top_sem, pair_sem,
):
    x, z, c = lax.axis_index(AX), lax.axis_index(AZ), lax.axis_index(AC)
    requests, width = q_ref.shape
    new_width = kv_ref.shape[1]
    slots, block = k_hbm.shape[0], k_hbm.shape[1]
    xc = NX * NC
    zh, zl = z // 2, z % 2
    mine_d = c * 2 + zl
    mine = x * 4 + mine_d
    scale = DH**-0.5

    top_z = NZ - 1
    small = [
        pltpu.make_async_copy(src, dst, small_sem.at[i])
        for i, (src, dst) in enumerate(
            ((q_hbm, q_ref), (kv_hbm, kv_ref), (req_hbm, req_ref), (len_hbm, len_ref))
        )
    ]
    small[0].start()
    small[1].start()
    barrier = pltpu.get_barrier_semaphore()
    others = [(dx, dc) for dx in FAR_X + (0,) for dc in range(NC) if dx or dc]

    def on_z(z_there):
        return at(x, z_there % NZ, c)

    def plane_mate(dx, dc, z_there):
        return at((x + dx) % NX, z_there % NZ, (c + dc) % NC)

    @pl.when((z > 0) & (z < top_z))
    def _():
        pl.semaphore_signal(barrier, 1, device_id=on_z(NZ), device_id_type=MESH)

    @pl.when(z == 1)
    def _():
        pl.semaphore_signal(barrier, 1, device_id=at(x, z, 1 - c), device_id_type=MESH)

    @pl.when(z == 0)
    def _():
        for dx, dc in others + [(0, 0)]:
            there = plane_mate(dx, dc, top_z)
            pl.semaphore_signal(barrier, 1, device_id=there, device_id_type=MESH)

    for i in FAR_Z:

        @pl.when((z > 0) & (z + i < NZ))
        def _(i=i):
            pl.semaphore_signal(barrier, 1, device_id=on_z(z + i), device_id_type=MESH)

    @pl.when((z > 0) & (z + 2 < NZ))
    def _():
        for dx, dc in others:
            there = plane_mate(dx, dc, z + 2)
            pl.semaphore_signal(barrier, 1, device_id=there, device_id_type=MESH)

    loads = []
    for s in range(slots):
        loads.append(pltpu.make_async_copy(k_hbm.at[s], kbuf.at[s], load_sem.at[s]))
    for s in range(slots):
        loads.append(pltpu.make_async_copy(v_hbm.at[s], vbuf.at[s], load_sem.at[slots + s]))
    for load in small[2:] + loads:
        load.start()

    def as_row(ref, n):
        spread = (iota((n, LANES), 0) == iota((n, LANES), 1) % n).astype(BF16)
        wide = jnp.dot(ref[...], spread, preferred_element_type=F32)
        keep = iota((requests, LANES), 0) == iota((requests, LANES), 1) // n
        return jnp.sum(jnp.where(keep, wide, 0.0), axis=0, keepdims=True)

    place_z = zl * G + zh
    small[0].wait()
    small[1].wait()
    own = jnp.concatenate([as_row(q_ref, width), as_row(kv_ref, new_width)], axis=1)[None]
    above[pl.ds(place_z, 1)] = own

    def send(src, dst, phase, there, recv=None):
        pltpu.make_async_remote_copy(
            src_ref=src,
            dst_ref=dst,
            send_sem=send_sem.at[phase],
            recv_sem=recv_sem.at[phase] if recv is None else recv,
            device_id=there,
            device_id_type=MESH,
        ).start()

    greeted = z - 1 + jnp.where(z > 2, xc - 1, 0)
    greeted = greeted + jnp.where(z == top_z, xc, 0)
    pl.semaphore_wait(barrier, jnp.where(z == 0, NZ - 2, jnp.where(z == 1, 1, greeted)))

    row = above.at[place_z]

    def greeter(i):
        if i == 1:
            return z > 1
        return (z > i) | (z == 0) if i < top_z else (z == 0) | (z == top_z)

    for i in FAR_Z:

        @pl.when(greeter(i))
        def _(i=i):
            send(row, row, 8 + i, on_z(z + NZ - i), row_sem.at[z])

    @pl.when(z > 2)
    def _():
        pl.semaphore_signal(x_sem, 1, device_id=on_z(z + NZ - 2), device_id_type=MESH)

    @pl.when(z == top_z)
    def _():
        pl.semaphore_signal(x_sem, 1, device_id=on_z(NZ), device_id_type=MESH)

    @pl.when(z >= top_z - 1)
    def _():
        for dx, dc in others + [(0, 0)]:
            there = plane_mate(dx, dc, z + NZ - 2)
            pl.semaphore_signal(top_sem, 1, device_id=there, device_id_type=MESH)

    @pl.when((z == 1) | (z == 2))
    def _():
        below[...] = jnp.zeros_like(below)

    @pl.when((z > 0) & (z < top_z))
    def _():
        wait_for(row, row_sem.at[z + 1])
        send(row, row, 8 + NZ, on_z(z + 1), row_sem.at[z])

    @pl.when(z > 2)
    def _():
        wait_for(below, recv_sem.at[0])

    @pl.when(z > 1)
    def _():
        wait_for(row, row_sem.at[z - 1])
        below_z = (1 - zl) * G + (z - 1) // 2
        below[pl.ds(below_z, 1)] = above[pl.ds(below_z, 1)]

    @pl.when(z > 0)
    def _():
        below[pl.ds(place_z, 1)] = own

    @pl.when(z == top_z - 1)
    def _():
        wait_for(row, row_sem.at[0])
        send(below, below, 8, on_z(NZ), recv_sem.at[0])

    @pl.when((z > 0) & (z < top_z - 1))
    def _():
        wait_for(row, row_sem.at[z + 2])
        send(below, below, 0, on_z(z + 2), recv_sem.at[0])

    @pl.when(z == 0)
    def _():
        wait_for(row, row_sem.at[top_z])
        send(row, row, 9, on_z(top_z), row_sem.at[0])
        wait_for(below, recv_sem.at[0])

    small[2].wait()
    small[3].wait()
    req = [req_ref[s] for s in range(slots)]
    length = [len_ref[s] for s in range(slots)]
    lane512 = iota((LANES, 2 * NC * LANES), 1)
    sub512 = iota((LANES, 2 * NC * LANES), 0)
    place = []
    for cc in range(NC):
        m = lane512 % LANES
        want = jnp.where((lane512 // LANES) % 2 == 0, req[0], req[1]) * width + m % width
        piece = (lane512 // (2 * LANES)) * NC + cc
        place.append(((sub512 == want) & (m // width == piece)).astype(BF16))

    for i in range(3, NZ):

        @pl.when((z > 0) & (z + i < NZ))
        def _(i=i):
            wait_for(row, row_sem.at[z + i])

    @pl.when((z > 0) & (z != top_z - 1))
    def _():
        wait_for(row, row_sem.at[0])

    @pl.when((z >= top_z - 3) & (z < top_z - 1))
    def _():
        pl.semaphore_wait(top_sem, xc)
        pl.semaphore_signal(x_sem, 1, device_id=on_z(z + 2), device_id_type=MESH)

    z_of = iota((NZ, 2 * LANES), 0)
    z_of = 2 * (z_of % G) + z_of // G
    from_below = (z_of > 0) & (z_of < jnp.where(z == 0, top_z, z))
    rows = jnp.where(from_below, below[:, 0, :], above[:, 0, :]).astype(BF16)
    row1 = c * NX + x
    g2[pl.ds(row1, 1)] = rows[:, 0:LANES][None]
    kv2[pl.ds(row1, 1)] = rows[:, LANES : 2 * LANES][None]

    pl.semaphore_wait(x_sem, 1)
    for dx, dc in others:
        send(g2.at[row1], g2.at[row1], 1, plane_mate(dx, dc, z))
    pl.semaphore_signal(pair_sem, 1, device_id=at(x, 2 * zh + 1 - zl, c), device_id_type=MESH)
    for load in loads:
        load.wait()
    wait_for(g2.at[pl.ds(0, xc - 1)], recv_sem.at[1])

    picked = [None, None]
    for cc in range(NC):
        lhs = g2[cc * NX : (cc + 1) * NX].reshape(NX * NZ, LANES)
        placed = jnp.dot(lhs, place[cc], preferred_element_type=F32).reshape(NX, NZ, 4 * LANES)
        for s in range(slots):
            for zp in range(2):
                at_lane = (zp * 2 + s) * LANES
                part = placed[:, zp * G : (zp + 1) * G, at_lane : at_lane + LANES]
                picked[s] = part if picked[s] is None else picked[s] + part
    for s in range(slots):
        qscr[s] = picked[s].astype(BF16)
    pl.semaphore_wait(pair_sem, 1)

    lane = iota((G, LANES), 1)
    lane_s, lane_hh, lane_r = (lane // 8) % 2, (lane // 4) % 2, lane % 4
    inside = [iota((G, block), 1) < length[s] for s in range(slots)]
    order = FAR_X + (0,)
    weights, vals = {}, {}
    numbered = list(enumerate(order))
    for part in (numbered[0:3], numbered[3:]):
        for n, dx in part:
            k = (x + dx) % NX
            cols = pl.ds(pl.multiple_of(k * DH, DH), DH)
            tops, sums = [], []
            for s in range(slots):
                qk = qscr[s, k]
                sc = lax.dot_general(
                    qk, kbuf[s, :, cols], (((1,), (1,)), ((), ())), preferred_element_type=F32
                )
                sc = jnp.where(inside[s], sc * scale, NEG)
                top = jnp.max(sc, axis=1, keepdims=True)
                w = jnp.exp(sc - top)
                tops.append(top)
                sums.append(jnp.sum(w, axis=1, keepdims=True))
                weights[n, s] = w.astype(BF16)
            of_slot = [
                jnp.where(
                    lane < 64,
                    jnp.where(lane_r == req[s], tops[s], NEG),
                    jnp.where(lane_r == req[s], sums[s], 0.0),
                )
                for s in range(slots)
            ]
            vals[n] = jnp.where(lane_s == 0, of_slot[0], of_slot[1])
        for n, dx in part:
            k = (x + dx) % NX
            cols = pl.ds(pl.multiple_of(k * DH, DH), DH)
            for d in range(4):
                sml[n, d] = jnp.where(
                    lane_hh[0:1] == 0, vals[n][2 * d : 2 * d + 1], vals[n][2 * d + 1 : 2 * d + 2]
                )
            for s in range(slots):
                o = jnp.dot(weights[n, s], vbuf[s, :, cols], preferred_element_type=F32)
                for d in range(4):
                    so[n, d, 2 * s : 2 * s + 2, :] = o[2 * d : 2 * d + 2]
            for dd in range(4):
                if dx or dd:
                    d = dd if dx else (mine_d + dd) % 4
                    there = at(k, 2 * zh + d % 2, d // 2)
                    send(sml.at[n, d], rml.at[mine], 4, there)
                    send(so.at[n, d], ro.at[mine], 3, there)
    last = len(order) - 1
    ro[pl.ds(mine, 1)] = so[last, pl.ds(mine_d, 1)]
    rml[pl.ds(mine, 1)] = sml[last, pl.ds(mine_d, 1)]

    for dx, dc in others:
        send(kv2.at[row1], kv2.at[row1], 2, plane_mate(dx, dc, z))

    group = 4 * NX
    wait_for(rml.at[pl.ds(0, group - 1)], recv_sem.at[4])
    ml = rml[:, 0, :]
    top = jnp.max(ml, axis=0, keepdims=True)
    top = jnp.maximum(top, pltpu.roll(top, 8, 1))
    w = jnp.exp(ml - top)
    total = jnp.sum(w * pltpu.roll(ml, 64, 1), axis=0, keepdims=True)
    total = total + pltpu.roll(total, 8, 1)
    lane1 = iota((1, LANES), 1)
    aml[pl.ds(z, 1)] = jnp.where(lane1 < 64, top, pltpu.roll(total, 64, 1))[None]
    wait_for(ro.at[pl.ds(0, group - 1)], recv_sem.at[3])
    merged = []
    for hh in range(2):
        planes = [ro[:, s * 2 + hh, :] for s in range(slots)]
        for r in range(requests):
            acc = None
            for s in range(slots):
                i = 16 + s * 8 + hh * 4 + r
                part = w[:, i : i + 1] * planes[s]
                acc = part if acc is None else acc + part
            merged.append(jnp.sum(acc, axis=0, keepdims=True))
    ao[pl.ds(z, 1)] = jnp.concatenate(merged, axis=0)[None]

    for i in range(NZ):

        @pl.when(z != i)
        def _(i=i):
            send(aml.at[z], aml.at[z], 6, on_z(i))
            send(ao.at[z], ao.at[z], 5, on_z(i))

    wait_for(kv2.at[pl.ds(0, xc - 1)], recv_sem.at[2])
    total_rows = NZ * xc
    u, col = iota((2 * xc, total_rows), 0), iota((2 * xc, total_rows), 1)
    zi = (u % xc) // NC
    from_row = (u % NC) * NX + x // 2 + (NX // 2) * (u // xc)
    source = from_row * NZ + (zi % 2) * G + (x % 2) * (G // 2) + zi // 2
    pick = (col == source).astype(BF16)
    new = jnp.dot(pick, kv2[...].reshape(total_rows, LANES), preferred_element_type=F32)
    wide_l, wide_m = iota((LANES, requests * LANES), 0), iota((LANES, requests * LANES), 1)
    wide_r, wide_m = wide_m // LANES, wide_m % LANES
    to_new = (wide_l == wide_r * new_width + wide_m % new_width).astype(BF16)
    to_q = (wide_l == wide_r * width + wide_m % width).astype(BF16)
    new = jnp.dot(new.astype(BF16), to_new, preferred_element_type=F32)
    keep = (iota(new.shape, 1) % LANES) // new_width == iota(new.shape, 0) % xc
    new = jnp.where(keep, new, 0.0)

    def by_request(flat):
        return [flat[:, r * LANES : (r + 1) * LANES] for r in range(requests)]

    new_k = by_request(jnp.sum(new[0:xc], axis=0, keepdims=True))
    new_v = by_request(jnp.sum(new[xc : 2 * xc], axis=0, keepdims=True))
    u, col = iota((16, total_rows), 0), iota((16, total_rows), 1)
    source = ((u % NC) * NX + x) * NZ + ((u % 4) // NC) * G + 4 * c + u // 4
    pick = (col == source).astype(BF16)
    own_q = jnp.dot(pick, g2[...].reshape(total_rows, LANES), preferred_element_type=F32)
    own_q = jnp.dot(own_q.astype(BF16), to_q, preferred_element_type=F32)
    keep = (iota(own_q.shape, 1) % LANES) // width == iota(own_q.shape, 0) % 4
    own_q = jnp.where(keep, own_q, 0.0)
    k_rows = jnp.concatenate(new_k + new_k, axis=0)
    v_rows = jnp.concatenate(new_v + new_v, axis=0)
    new_score = []
    for half in range(2):
        q_rows = []
        for hh in range(2):
            i = (half * 2 + hh) * 4
            q_rows += by_request(jnp.sum(own_q[i : i + 4], axis=0, keepdims=True))
        q_rows = jnp.concatenate(q_rows, axis=0)
        new_score.append(jnp.sum(q_rows * k_rows, axis=1, keepdims=True) * scale)

    wait_for(aml.at[pl.ds(0, NZ - 1)], recv_sem.at[6])
    sub = iota((8, LANES), 0)
    lane8 = iota((8, LANES), 1)
    m_at, l_at = lane8 == 16 + sub, lane8 == 80 + sub
    ways = []
    for half in range(2):
        planes = range(half, NZ, 2)
        ms = [jnp.sum(jnp.where(m_at, aml[i], 0.0), axis=1, keepdims=True) for i in planes]
        ls = [jnp.sum(jnp.where(l_at, aml[i], 0.0), axis=1, keepdims=True) for i in planes]
        peak = functools.reduce(jnp.maximum, ms, new_score[half])
        new_w = jnp.exp(new_score[half] - peak)
        factors = [jnp.exp(m - peak) for m in ms]
        denom = new_w
        for factor, part in zip(factors, ls):
            denom = denom + factor * part
        ways.append((new_w, factors, denom))
    wait_for(ao.at[pl.ds(0, NZ - 1)], recv_sem.at[5])
    base = pl.multiple_of((x * NC + c) * 4 * DH, 4 * DH)
    for half in range(2):
        new_w, factors, denom = ways[half]
        numer = new_w * v_rows
        for i, factor in zip(range(half, NZ, 2), factors):
            numer = numer + factor * ao[i]
        final = (numer / denom).astype(BF16)
        for hh in range(2):
            start = pl.multiple_of(base + (half * 2 + hh) * DH, DH)
            out_ref[:, pl.ds(start, DH)] = final[hh * 4 : hh * 4 + 4]

    here = out_ref.at[:, pl.ds(base, 4 * DH)]
    for dx, dc in others:
        send(here, here, 7, plane_mate(dx, dc, z))
    wait_for(out_ref.at[:, pl.ds(0, (xc - 1) * 4 * DH)], recv_sem.at[7])

    for i in range(1, NZ):

        @pl.when(greeter(i) if i > 1 else z != 1)
        def _(i=i):
            wait_for(row, send_sem.at[8 + i])

    @pl.when((z > 0) & (z < top_z))
    def _():
        wait_for(row, send_sem.at[8 + NZ])

    @pl.when((z > 0) & (z < top_z - 1))
    def _():
        wait_for(below, send_sem.at[0])

    @pl.when(z == top_z - 1)
    def _():
        wait_for(below, send_sem.at[8])

    wait_for(g2.at[pl.ds(0, xc - 1)], send_sem.at[1])
    wait_for(kv2.at[pl.ds(0, xc - 1)], send_sem.at[2])
    wait_for(ro.at[pl.ds(0, group - 1)], send_sem.at[3])
    wait_for(rml.at[pl.ds(0, group - 1)], send_sem.at[4])
    wait_for(ao.at[pl.ds(0, NZ - 1)], send_sem.at[5])
    wait_for(aml.at[pl.ds(0, NZ - 1)], send_sem.at[6])
    wait_for(out_ref.at[:, pl.ds(0, (xc - 1) * 4 * DH)], send_sem.at[7])


def shards(queries, new_kv, keys, values, slot_request, slot_length):
    slots, block, columns = keys.shape
    requests = queries.shape[0]
    xc, group = NX * NC, 4 * NX
    vmem = pl.BlockSpec(memory_space=pltpu.VMEM)
    hbm = pl.BlockSpec(memory_space=pl.ANY)
    return pl.pallas_call(
        kernel,
        out_shape=pltpu.VMEM((requests, H * DH), BF16),
        in_specs=[hbm] * 6,
        out_specs=vmem,
        scratch_shapes=[
            pltpu.SMEM(slot_request.shape, jnp.int32),
            pltpu.SMEM(slot_length.shape, jnp.int32),
            pltpu.VMEM(queries.shape, BF16),
            pltpu.VMEM(new_kv.shape, BF16),
            pltpu.VMEM((slots, block, columns), BF16),
            pltpu.VMEM((slots, block, columns), BF16),
            pltpu.VMEM((NZ, 1, 2 * LANES), F32),
            pltpu.VMEM((NZ, 1, 2 * LANES), F32),
            pltpu.VMEM((xc, NZ, LANES), BF16),
            pltpu.VMEM((xc, NZ, LANES), BF16),
            pltpu.VMEM((slots, KVH, G, DH), BF16),
            pltpu.VMEM((KVH, 4, 4, DH), F32),
            pltpu.VMEM((KVH, 4, 1, LANES), F32),
            pltpu.VMEM((group, 4, DH), F32),
            pltpu.VMEM((group, 1, LANES), F32),
            pltpu.VMEM((NZ, 8, DH), F32),
            pltpu.VMEM((NZ, 1, LANES), F32),
            pltpu.SemaphoreType.DMA((2 * slots,)),
            pltpu.SemaphoreType.DMA((4,)),
            pltpu.SemaphoreType.DMA((9 + NZ,)),
            pltpu.SemaphoreType.DMA((8,)),
            pltpu.SemaphoreType.DMA((NZ,)),
            pltpu.SemaphoreType.REGULAR,
            pltpu.SemaphoreType.REGULAR,
            pltpu.SemaphoreType.REGULAR,
        ],
        compiler_params=pltpu.CompilerParams(collective_id=0, has_side_effects=True),
        cost_estimate=pl.CostEstimate(
            flops=4 * slots * block * H * DH,
            bytes_accessed=4 * slots * block * columns,
            transcendentals=slots * block * H,
        ),
        name="decode",
    )(slot_request, slot_length, queries, new_kv, keys, values)


def solution(mesh):
    torus = Mesh(mesh.devices.reshape(mesh.shape["parts"], NX, NZ, NC), ("parts",) + SEQ)
    placed = (
        P("parts", SEQ),
        P("parts", SEQ),
        P(PARTS_SEQ, None, None),
        P(PARTS_SEQ, None, None),
        P(PARTS_SEQ),
        P(PARTS_SEQ),
    )
    return jax.shard_map(
        shards, mesh=torus, in_specs=placed, out_specs=P("parts", None), check_vma=False
    )
```

```python
import functools

import jax
import jax.numpy as jnp
from jax import lax
from jax.experimental import pallas as pl
from jax.experimental.pallas import tpu as pltpu
from jax.sharding import Mesh
from jax.sharding import PartitionSpec as P

H = 64
KVH = 8
DH = 128
G = H // KVH
LANES = 128
NX, NZ, NC = 8, 16, 2
AX, AZ, AC = "seq_0", "seq_1", "seq_2"
SEQ = (AX, AZ, AC)
PARTS_SEQ = ("parts", AX, AZ, AC)
NEG = -1e30
MESH = pl.DeviceIdType.MESH
F32, BF16 = jnp.float32, jnp.bfloat16
FAR_X = (4, 3, 5, 2, 6, 1, 7)
FAR_Z = (8, 7, 9, 6, 10, 5, 11, 4, 12, 3, 13, 2, 14, 1, 15)


def iota(shape, dim):
    return lax.broadcasted_iota(jnp.int32, shape, dim)


def at(x, z, c):
    return {AX: x, AZ: z, AC: c}


def wait_for(ref, sem):
    pltpu.make_async_copy(ref, ref, sem).wait()


def kernel(
    req_hbm, len_hbm, q_hbm, kv_hbm, k_hbm, v_hbm, out_ref,
    req_ref, len_ref, q_ref, kv_ref, kbuf, vbuf, above, below, g2, kv2, qscr, so, sml, ro, rml, ao, aml,
    load_sem, small_sem, send_sem, recv_sem, row_sem, x_sem, top_sem, pair_sem,
):
    x, z, c = lax.axis_index(AX), lax.axis_index(AZ), lax.axis_index(AC)
    requests, width = q_ref.shape
    new_width = kv_ref.shape[1]
    slots, block = k_hbm.shape[0], k_hbm.shape[1]
    xc = NX * NC
    zh, zl = z // 2, z % 2
    mine_d = c * 2 + zl
    mine = x * 4 + mine_d
    scale = DH**-0.5

    top_z = NZ - 1
    small = [
        pltpu.make_async_copy(src, dst, small_sem.at[i])
        for i, (src, dst) in enumerate(
            ((q_hbm, q_ref), (kv_hbm, kv_ref), (req_hbm, req_ref), (len_hbm, len_ref))
        )
    ]
    small[0].start()
    small[1].start()
    barrier = pltpu.get_barrier_semaphore()
    others = [(dx, dc) for dx in FAR_X + (0,) for dc in range(NC) if dx or dc]

    def on_z(z_there):
        return at(x, z_there % NZ, c)

    def plane_mate(dx, dc, z_there):
        return at((x + dx) % NX, z_there % NZ, (c + dc) % NC)

    @pl.when((z > 0) & (z < top_z))
    def _():
        pl.semaphore_signal(barrier, 1, device_id=on_z(NZ), device_id_type=MESH)

    @pl.when(z == 1)
    def _():
        pl.semaphore_signal(barrier, 1, device_id=at(x, z, 1 - c), device_id_type=MESH)

    @pl.when(z == 0)
    def _():
        for dx, dc in others + [(0, 0)]:
            there = plane_mate(dx, dc, top_z)
            pl.semaphore_signal(barrier, 1, device_id=there, device_id_type=MESH)

    for i in FAR_Z:

        @pl.when((z > 0) & (z + i < NZ))
        def _(i=i):
            pl.semaphore_signal(barrier, 1, device_id=on_z(z + i), device_id_type=MESH)

    @pl.when((z > 0) & (z + 2 < NZ))
    def _():
        for dx, dc in others:
            there = plane_mate(dx, dc, z + 2)
            pl.semaphore_signal(barrier, 1, device_id=there, device_id_type=MESH)

    loads = []
    for s in range(slots):
        loads.append(pltpu.make_async_copy(k_hbm.at[s], kbuf.at[s], load_sem.at[s]))
    for s in range(slots):
        loads.append(pltpu.make_async_copy(v_hbm.at[s], vbuf.at[s], load_sem.at[slots + s]))
    for load in small[2:] + loads:
        load.start()

    def as_row(ref, n):
        spread = (iota((n, LANES), 0) == iota((n, LANES), 1) % n).astype(BF16)
        wide = jnp.dot(ref[...], spread, preferred_element_type=F32)
        keep = iota((requests, LANES), 0) == iota((requests, LANES), 1) // n
        return jnp.sum(jnp.where(keep, wide, 0.0), axis=0, keepdims=True)

    place_z = zl * G + zh
    small[0].wait()
    small[1].wait()
    own = jnp.concatenate([as_row(q_ref, width), as_row(kv_ref, new_width)], axis=1)[None]
    above[pl.ds(place_z, 1)] = own

    def send(src, dst, phase, there, recv=None):
        pltpu.make_async_remote_copy(
            src_ref=src,
            dst_ref=dst,
            send_sem=send_sem.at[phase],
            recv_sem=recv_sem.at[phase] if recv is None else recv,
            device_id=there,
            device_id_type=MESH,
        ).start()

    greeted = z - 1 + jnp.where(z > 2, xc - 1, 0)
    greeted = greeted + jnp.where(z == top_z, xc, 0)
    pl.semaphore_wait(barrier, jnp.where(z == 0, NZ - 2, jnp.where(z == 1, 1, greeted)))

    row = above.at[place_z]

    def greeter(i):
        if i == 1:
            return z > 1
        return (z > i) | (z == 0) if i < top_z else (z == 0) | (z == top_z)

    for i in FAR_Z:

        @pl.when(greeter(i))
        def _(i=i):
            send(row, row, 8 + i, on_z(z + NZ - i), row_sem.at[z])

    @pl.when(z > 2)
    def _():
        pl.semaphore_signal(x_sem, 1, device_id=on_z(z + NZ - 2), device_id_type=MESH)

    @pl.when(z == top_z)
    def _():
        pl.semaphore_signal(x_sem, 1, device_id=on_z(NZ), device_id_type=MESH)

    @pl.when(z >= top_z - 1)
    def _():
        for dx, dc in others + [(0, 0)]:
            there = plane_mate(dx, dc, z + NZ - 2)
            pl.semaphore_signal(top_sem, 1, device_id=there, device_id_type=MESH)

    @pl.when((z == 1) | (z == 2))
    def _():
        below[...] = jnp.zeros_like(below)

    @pl.when((z > 0) & (z < top_z))
    def _():
        wait_for(row, row_sem.at[z + 1])
        send(row, row, 8 + NZ, on_z(z + 1), row_sem.at[z])

    @pl.when(z > 2)
    def _():
        wait_for(below, recv_sem.at[0])

    @pl.when(z > 1)
    def _():
        wait_for(row, row_sem.at[z - 1])
        below_z = (1 - zl) * G + (z - 1) // 2
        below[pl.ds(below_z, 1)] = above[pl.ds(below_z, 1)]

    @pl.when(z > 0)
    def _():
        below[pl.ds(place_z, 1)] = own

    @pl.when(z == top_z - 1)
    def _():
        wait_for(row, row_sem.at[0])
        send(below, below, 8, on_z(NZ), recv_sem.at[0])

    @pl.when((z > 0) & (z < top_z - 1))
    def _():
        wait_for(row, row_sem.at[z + 2])
        send(below, below, 0, on_z(z + 2), recv_sem.at[0])

    @pl.when(z == 0)
    def _():
        wait_for(row, row_sem.at[top_z])
        send(row, row, 9, on_z(top_z), row_sem.at[0])
        wait_for(below, recv_sem.at[0])

    small[2].wait()
    small[3].wait()
    req = [req_ref[s] for s in range(slots)]
    length = [len_ref[s] for s in range(slots)]
    lane512 = iota((LANES, 2 * NC * LANES), 1)
    sub512 = iota((LANES, 2 * NC * LANES), 0)
    place = []
    for cc in range(NC):
        m = lane512 % LANES
        want = jnp.where((lane512 // LANES) % 2 == 0, req[0], req[1]) * width + m % width
        piece = (lane512 // (2 * LANES)) * NC + cc
        place.append(((sub512 == want) & (m // width == piece)).astype(BF16))

    for i in range(3, NZ):

        @pl.when((z > 0) & (z + i < NZ))
        def _(i=i):
            wait_for(row, row_sem.at[z + i])

    @pl.when((z > 0) & (z != top_z - 1))
    def _():
        wait_for(row, row_sem.at[0])

    @pl.when((z >= top_z - 3) & (z < top_z - 1))
    def _():
        pl.semaphore_wait(top_sem, xc)
        pl.semaphore_signal(x_sem, 1, device_id=on_z(z + 2), device_id_type=MESH)

    z_of = iota((NZ, 2 * LANES), 0)
    z_of = 2 * (z_of % G) + z_of // G
    from_below = (z_of > 0) & (z_of < jnp.where(z == 0, top_z, z))
    rows = jnp.where(from_below, below[:, 0, :], above[:, 0, :]).astype(BF16)
    row1 = c * NX + x
    g2[pl.ds(row1, 1)] = rows[:, 0:LANES][None]
    kv2[pl.ds(row1, 1)] = rows[:, LANES : 2 * LANES][None]

    pl.semaphore_wait(x_sem, 1)
    for dx, dc in others:
        send(g2.at[row1], g2.at[row1], 1, plane_mate(dx, dc, z))
    pl.semaphore_signal(pair_sem, 1, device_id=at(x, 2 * zh + 1 - zl, c), device_id_type=MESH)
    for load in loads:
        load.wait()
    wait_for(g2.at[pl.ds(0, xc - 1)], recv_sem.at[1])

    picked = [None, None]
    for cc in range(NC):
        lhs = g2[cc * NX : (cc + 1) * NX].reshape(NX * NZ, LANES)
        placed = jnp.dot(lhs, place[cc], preferred_element_type=F32).reshape(NX, NZ, 4 * LANES)
        for s in range(slots):
            for zp in range(2):
                at_lane = (zp * 2 + s) * LANES
                part = placed[:, zp * G : (zp + 1) * G, at_lane : at_lane + LANES]
                picked[s] = part if picked[s] is None else picked[s] + part
    for s in range(slots):
        qscr[s] = picked[s].astype(BF16)
    pl.semaphore_wait(pair_sem, 1)

    lane = iota((G, LANES), 1)
    lane_s, lane_hh, lane_r = (lane // 8) % 2, (lane // 4) % 2, lane % 4
    inside = [iota((G, block), 1) < length[s] for s in range(slots)]
    order = FAR_X + (0,)
    weights, vals = {}, {}
    numbered = list(enumerate(order))
    for part in (numbered[0:3], numbered[3:]):
        for n, dx in part:
            k = (x + dx) % NX
            cols = pl.ds(pl.multiple_of(k * DH, DH), DH)
            tops, sums = [], []
            for s in range(slots):
                qk = qscr[s, k]
                sc = lax.dot_general(
                    qk, kbuf[s, :, cols], (((1,), (1,)), ((), ())), preferred_element_type=F32
                )
                sc = jnp.where(inside[s], sc * scale, NEG)
                top = jnp.max(sc, axis=1, keepdims=True)
                w = jnp.exp(sc - top)
                tops.append(top)
                sums.append(jnp.sum(w, axis=1, keepdims=True))
                weights[n, s] = w.astype(BF16)
            of_slot = [
                jnp.where(
                    lane < 64,
                    jnp.where(lane_r == req[s], tops[s], NEG),
                    jnp.where(lane_r == req[s], sums[s], 0.0),
                )
                for s in range(slots)
            ]
            vals[n] = jnp.where(lane_s == 0, of_slot[0], of_slot[1])
        for n, dx in part:
            k = (x + dx) % NX
            cols = pl.ds(pl.multiple_of(k * DH, DH), DH)
            for d in range(4):
                sml[n, d] = jnp.where(
                    lane_hh[0:1] == 0, vals[n][2 * d : 2 * d + 1], vals[n][2 * d + 1 : 2 * d + 2]
                )
            o = [
                jnp.dot(weights[n, s], vbuf[s, :, cols], preferred_element_type=F32)
                for s in range(slots)
            ]
            for d in range(4):
                four = jnp.concatenate([o[s][2 * d : 2 * d + 2] for s in range(slots)], axis=0)
                so[n, d] = four.astype(BF16)
            for dd in range(4):
                if dx or dd:
                    d = dd if dx else (mine_d + dd) % 4
                    there = at(k, 2 * zh + d % 2, d // 2)
                    send(sml.at[n, d], rml.at[mine], 4, there)
                    send(so.at[n, d], ro.at[mine], 3, there)
    last = len(order) - 1
    ro[pl.ds(mine, 1)] = so[last, pl.ds(mine_d, 1)]
    rml[pl.ds(mine, 1)] = sml[last, pl.ds(mine_d, 1)]

    for dx, dc in others:
        send(kv2.at[row1], kv2.at[row1], 2, plane_mate(dx, dc, z))

    group = 4 * NX
    wait_for(rml.at[pl.ds(0, group - 1)], recv_sem.at[4])
    ml = rml[:, 0, :]
    top = jnp.max(ml, axis=0, keepdims=True)
    top = jnp.maximum(top, pltpu.roll(top, 8, 1))
    w = jnp.exp(ml - top)
    total = jnp.sum(w * pltpu.roll(ml, 64, 1), axis=0, keepdims=True)
    total = total + pltpu.roll(total, 8, 1)
    lane1 = iota((1, LANES), 1)
    aml[pl.ds(z, 1)] = jnp.where(lane1 < 64, top, pltpu.roll(total, 64, 1))[None]
    wait_for(ro.at[pl.ds(0, group - 1)], recv_sem.at[3])
    got = ro[...].astype(F32)
    merged = []
    for hh in range(2):
        planes = [got[:, s * 2 + hh, :] for s in range(slots)]
        for r in range(requests):
            acc = None
            for s in range(slots):
                i = 16 + s * 8 + hh * 4 + r
                part = w[:, i : i + 1] * planes[s]
                acc = part if acc is None else acc + part
            merged.append(jnp.sum(acc, axis=0, keepdims=True))
    ao[pl.ds(z, 1)] = jnp.concatenate(merged, axis=0).astype(BF16)[None]

    for i in range(NZ):

        @pl.when(z != i)
        def _(i=i):
            send(aml.at[z], aml.at[z], 6, on_z(i))
            send(ao.at[z], ao.at[z], 5, on_z(i))

    wait_for(kv2.at[pl.ds(0, xc - 1)], recv_sem.at[2])
    total_rows = NZ * xc
    u, col = iota((2 * xc, total_rows), 0), iota((2 * xc, total_rows), 1)
    zi = (u % xc) // NC
    from_row = (u % NC) * NX + x // 2 + (NX // 2) * (u // xc)
    source = from_row * NZ + (zi % 2) * G + (x % 2) * (G // 2) + zi // 2
    pick = (col == source).astype(BF16)
    new = jnp.dot(pick, kv2[...].reshape(total_rows, LANES), preferred_element_type=F32)
    wide_l, wide_m = iota((LANES, requests * LANES), 0), iota((LANES, requests * LANES), 1)
    wide_r, wide_m = wide_m // LANES, wide_m % LANES
    to_new = (wide_l == wide_r * new_width + wide_m % new_width).astype(BF16)
    to_q = (wide_l == wide_r * width + wide_m % width).astype(BF16)
    new = jnp.dot(new.astype(BF16), to_new, preferred_element_type=F32)
    keep = (iota(new.shape, 1) % LANES) // new_width == iota(new.shape, 0) % xc
    new = jnp.where(keep, new, 0.0)

    def by_request(flat):
        return [flat[:, r * LANES : (r + 1) * LANES] for r in range(requests)]

    new_k = by_request(jnp.sum(new[0:xc], axis=0, keepdims=True))
    new_v = by_request(jnp.sum(new[xc : 2 * xc], axis=0, keepdims=True))
    u, col = iota((16, total_rows), 0), iota((16, total_rows), 1)
    source = ((u % NC) * NX + x) * NZ + ((u % 4) // NC) * G + 4 * c + u // 4
    pick = (col == source).astype(BF16)
    own_q = jnp.dot(pick, g2[...].reshape(total_rows, LANES), preferred_element_type=F32)
    own_q = jnp.dot(own_q.astype(BF16), to_q, preferred_element_type=F32)
    keep = (iota(own_q.shape, 1) % LANES) // width == iota(own_q.shape, 0) % 4
    own_q = jnp.where(keep, own_q, 0.0)
    k_rows = jnp.concatenate(new_k + new_k, axis=0)
    v_rows = jnp.concatenate(new_v + new_v, axis=0)
    new_score = []
    for half in range(2):
        q_rows = []
        for hh in range(2):
            i = (half * 2 + hh) * 4
            q_rows += by_request(jnp.sum(own_q[i : i + 4], axis=0, keepdims=True))
        q_rows = jnp.concatenate(q_rows, axis=0)
        new_score.append(jnp.sum(q_rows * k_rows, axis=1, keepdims=True) * scale)

    wait_for(aml.at[pl.ds(0, NZ - 1)], recv_sem.at[6])
    sub = iota((8, LANES), 0)
    lane8 = iota((8, LANES), 1)
    m_at, l_at = lane8 == 16 + sub, lane8 == 80 + sub
    ways = []
    for half in range(2):
        planes = range(half, NZ, 2)
        ms = [jnp.sum(jnp.where(m_at, aml[i], 0.0), axis=1, keepdims=True) for i in planes]
        ls = [jnp.sum(jnp.where(l_at, aml[i], 0.0), axis=1, keepdims=True) for i in planes]
        peak = functools.reduce(jnp.maximum, ms, new_score[half])
        new_w = jnp.exp(new_score[half] - peak)
        factors = [jnp.exp(m - peak) for m in ms]
        denom = new_w
        for factor, part in zip(factors, ls):
            denom = denom + factor * part
        ways.append((new_w, factors, denom))
    wait_for(ao.at[pl.ds(0, NZ - 1)], recv_sem.at[5])
    base = pl.multiple_of((x * NC + c) * 4 * DH, 4 * DH)
    for half in range(2):
        new_w, factors, denom = ways[half]
        numer = new_w * v_rows
        for i, factor in zip(range(half, NZ, 2), factors):
            numer = numer + factor * ao[i].astype(F32)
        final = (numer / denom).astype(BF16)
        for hh in range(2):
            start = pl.multiple_of(base + (half * 2 + hh) * DH, DH)
            out_ref[:, pl.ds(start, DH)] = final[hh * 4 : hh * 4 + 4]

    here = out_ref.at[:, pl.ds(base, 4 * DH)]
    for dx, dc in others:
        send(here, here, 7, plane_mate(dx, dc, z))
    wait_for(out_ref.at[:, pl.ds(0, (xc - 1) * 4 * DH)], recv_sem.at[7])

    for i in range(1, NZ):

        @pl.when(greeter(i) if i > 1 else z != 1)
        def _(i=i):
            wait_for(row, send_sem.at[8 + i])

    @pl.when((z > 0) & (z < top_z))
    def _():
        wait_for(row, send_sem.at[8 + NZ])

    @pl.when((z > 0) & (z < top_z - 1))
    def _():
        wait_for(below, send_sem.at[0])

    @pl.when(z == top_z - 1)
    def _():
        wait_for(below, send_sem.at[8])

    wait_for(g2.at[pl.ds(0, xc - 1)], send_sem.at[1])
    wait_for(kv2.at[pl.ds(0, xc - 1)], send_sem.at[2])
    wait_for(ro.at[pl.ds(0, group - 1)], send_sem.at[3])
    wait_for(rml.at[pl.ds(0, group - 1)], send_sem.at[4])
    wait_for(ao.at[pl.ds(0, NZ - 1)], send_sem.at[5])
    wait_for(aml.at[pl.ds(0, NZ - 1)], send_sem.at[6])
    wait_for(out_ref.at[:, pl.ds(0, (xc - 1) * 4 * DH)], send_sem.at[7])


def shards(queries, new_kv, keys, values, slot_request, slot_length):
    slots, block, columns = keys.shape
    requests = queries.shape[0]
    xc, group = NX * NC, 4 * NX
    vmem = pl.BlockSpec(memory_space=pltpu.VMEM)
    hbm = pl.BlockSpec(memory_space=pl.ANY)
    return pl.pallas_call(
        kernel,
        out_shape=pltpu.VMEM((requests, H * DH), BF16),
        in_specs=[hbm] * 6,
        out_specs=vmem,
        scratch_shapes=[
            pltpu.SMEM(slot_request.shape, jnp.int32),
            pltpu.SMEM(slot_length.shape, jnp.int32),
            pltpu.VMEM(queries.shape, BF16),
            pltpu.VMEM(new_kv.shape, BF16),
            pltpu.VMEM((slots, block, columns), BF16),
            pltpu.VMEM((slots, block, columns), BF16),
            pltpu.VMEM((NZ, 1, 2 * LANES), F32),
            pltpu.VMEM((NZ, 1, 2 * LANES), F32),
            pltpu.VMEM((xc, NZ, LANES), BF16),
            pltpu.VMEM((xc, NZ, LANES), BF16),
            pltpu.VMEM((slots, KVH, G, DH), BF16),
            pltpu.VMEM((KVH, 4, 4, DH), BF16),
            pltpu.VMEM((KVH, 4, 1, LANES), F32),
            pltpu.VMEM((group, 4, DH), BF16),
            pltpu.VMEM((group, 1, LANES), F32),
            pltpu.VMEM((NZ, 8, DH), BF16),
            pltpu.VMEM((NZ, 1, LANES), F32),
            pltpu.SemaphoreType.DMA((2 * slots,)),
            pltpu.SemaphoreType.DMA((4,)),
            pltpu.SemaphoreType.DMA((9 + NZ,)),
            pltpu.SemaphoreType.DMA((8,)),
            pltpu.SemaphoreType.DMA((NZ,)),
            pltpu.SemaphoreType.REGULAR,
            pltpu.SemaphoreType.REGULAR,
            pltpu.SemaphoreType.REGULAR,
        ],
        compiler_params=pltpu.CompilerParams(collective_id=0, has_side_effects=True),
        cost_estimate=pl.CostEstimate(
            flops=4 * slots * block * H * DH,
            bytes_accessed=4 * slots * block * columns,
            transcendentals=slots * block * H,
        ),
        name="decode",
    )(slot_request, slot_length, queries, new_kv, keys, values)


def solution(mesh):
    torus = Mesh(mesh.devices.reshape(mesh.shape["parts"], NX, NZ, NC), ("parts",) + SEQ)
    placed = (
        P("parts", SEQ),
        P("parts", SEQ),
        P(PARTS_SEQ, None, None),
        P(PARTS_SEQ, None, None),
        P(PARTS_SEQ),
        P(PARTS_SEQ),
    )
    return jax.shard_map(
        shards, mesh=torus, in_specs=placed, out_specs=P("parts", None), check_vma=False
    )
```

```python
import functools

import jax
import jax.numpy as jnp
from jax import lax
from jax.experimental import pallas as pl
from jax.experimental.pallas import tpu as pltpu
from jax.sharding import Mesh
from jax.sharding import PartitionSpec as P

H = 64
KVH = 8
DH = 128
G = H // KVH
LANES = 128
NX, NZ, NC = 8, 16, 2
AX, AZ, AC = "seq_0", "seq_1", "seq_2"
SEQ = (AX, AZ, AC)
PARTS_SEQ = ("parts", AX, AZ, AC)
NEG = -1e30
MESH = pl.DeviceIdType.MESH
F32, BF16 = jnp.float32, jnp.bfloat16
FAR_X = (4, 3, 5, 2, 6, 1, 7)
FAR_Z = (8, 7, 9, 6, 10, 5, 11, 4, 12, 3, 13, 2, 14, 1, 15)


def iota(shape, dim):
    return lax.broadcasted_iota(jnp.int32, shape, dim)


def at(x, z, c):
    return {AX: x, AZ: z, AC: c}


def wait_for(ref, sem):
    pltpu.make_async_copy(ref, ref, sem).wait()


def kernel(
    req_hbm, len_hbm, q_hbm, kv_hbm, k_hbm, v_hbm, out_ref,
    req_ref, len_ref, q_ref, kv_ref, kbuf, vbuf, above, below, g2, kv2, qscr, so, sml, ro, got, rml, ao, aml,
    load_sem, small_sem, send_sem, recv_sem, row_sem, x_sem, top_sem, pair_sem,
):
    x, z, c = lax.axis_index(AX), lax.axis_index(AZ), lax.axis_index(AC)
    requests, width = q_ref.shape
    new_width = kv_ref.shape[1]
    slots, block = k_hbm.shape[0], k_hbm.shape[1]
    xc = NX * NC
    zh, zl = z // 2, z % 2
    mine_d = c * 2 + zl
    mine = x * 4 + mine_d
    scale = DH**-0.5

    top_z = NZ - 1
    small = [
        pltpu.make_async_copy(src, dst, small_sem.at[i])
        for i, (src, dst) in enumerate(
            ((q_hbm, q_ref), (kv_hbm, kv_ref), (req_hbm, req_ref), (len_hbm, len_ref))
        )
    ]
    small[0].start()
    small[1].start()
    barrier = pltpu.get_barrier_semaphore()
    others = [(dx, dc) for dx in FAR_X + (0,) for dc in range(NC) if dx or dc]

    def on_z(z_there):
        return at(x, z_there % NZ, c)

    def plane_mate(dx, dc, z_there):
        return at((x + dx) % NX, z_there % NZ, (c + dc) % NC)

    @pl.when((z > 0) & (z < top_z))
    def _():
        pl.semaphore_signal(barrier, 1, device_id=on_z(NZ), device_id_type=MESH)

    @pl.when(z == 1)
    def _():
        pl.semaphore_signal(barrier, 1, device_id=at(x, z, 1 - c), device_id_type=MESH)

    @pl.when(z == 0)
    def _():
        for dx, dc in others + [(0, 0)]:
            there = plane_mate(dx, dc, top_z)
            pl.semaphore_signal(barrier, 1, device_id=there, device_id_type=MESH)

    for i in FAR_Z:

        @pl.when((z > 0) & (z + i < NZ))
        def _(i=i):
            pl.semaphore_signal(barrier, 1, device_id=on_z(z + i), device_id_type=MESH)

    @pl.when((z > 0) & (z + 2 < NZ))
    def _():
        for dx, dc in others:
            there = plane_mate(dx, dc, z + 2)
            pl.semaphore_signal(barrier, 1, device_id=there, device_id_type=MESH)

    loads = []
    for s in range(slots):
        loads.append(pltpu.make_async_copy(k_hbm.at[s], kbuf.at[s], load_sem.at[s]))
    for s in range(slots):
        loads.append(pltpu.make_async_copy(v_hbm.at[s], vbuf.at[s], load_sem.at[slots + s]))
    for load in small[2:] + loads:
        load.start()

    def as_row(ref, n):
        spread = (iota((n, LANES), 0) == iota((n, LANES), 1) % n).astype(BF16)
        wide = jnp.dot(ref[...], spread, preferred_element_type=F32)
        keep = iota((requests, LANES), 0) == iota((requests, LANES), 1) // n
        return jnp.sum(jnp.where(keep, wide, 0.0), axis=0, keepdims=True)

    place_z = zl * G + zh
    small[0].wait()
    small[1].wait()
    own = jnp.concatenate([as_row(q_ref, width), as_row(kv_ref, new_width)], axis=1)[None]
    above[pl.ds(place_z, 1)] = own

    def send(src, dst, phase, there, recv=None):
        pltpu.make_async_remote_copy(
            src_ref=src,
            dst_ref=dst,
            send_sem=send_sem.at[phase],
            recv_sem=recv_sem.at[phase] if recv is None else recv,
            device_id=there,
            device_id_type=MESH,
        ).start()

    greeted = z - 1 + jnp.where(z > 2, xc - 1, 0)
    greeted = greeted + jnp.where(z == top_z, xc, 0)
    pl.semaphore_wait(barrier, jnp.where(z == 0, NZ - 2, jnp.where(z == 1, 1, greeted)))

    row = above.at[place_z]

    def greeter(i):
        if i == 1:
            return z > 1
        return (z > i) | (z == 0) if i < top_z else (z == 0) | (z == top_z)

    for i in FAR_Z:

        @pl.when(greeter(i))
        def _(i=i):
            send(row, row, 8 + i, on_z(z + NZ - i), row_sem.at[z])

    @pl.when(z > 2)
    def _():
        pl.semaphore_signal(x_sem, 1, device_id=on_z(z + NZ - 2), device_id_type=MESH)

    @pl.when(z == top_z)
    def _():
        pl.semaphore_signal(x_sem, 1, device_id=on_z(NZ), device_id_type=MESH)

    @pl.when(z >= top_z - 1)
    def _():
        for dx, dc in others + [(0, 0)]:
            there = plane_mate(dx, dc, z + NZ - 2)
            pl.semaphore_signal(top_sem, 1, device_id=there, device_id_type=MESH)

    @pl.when((z == 1) | (z == 2))
    def _():
        below[...] = jnp.zeros_like(below)

    @pl.when((z > 0) & (z < top_z))
    def _():
        wait_for(row, row_sem.at[z + 1])
        send(row, row, 8 + NZ, on_z(z + 1), row_sem.at[z])

    @pl.when(z > 2)
    def _():
        wait_for(below, recv_sem.at[0])

    @pl.when(z > 1)
    def _():
        wait_for(row, row_sem.at[z - 1])
        below_z = (1 - zl) * G + (z - 1) // 2
        below[pl.ds(below_z, 1)] = above[pl.ds(below_z, 1)]

    @pl.when(z > 0)
    def _():
        below[pl.ds(place_z, 1)] = own

    @pl.when(z == top_z - 1)
    def _():
        wait_for(row, row_sem.at[0])
        send(below, below, 8, on_z(NZ), recv_sem.at[0])

    @pl.when((z > 0) & (z < top_z - 1))
    def _():
        wait_for(row, row_sem.at[z + 2])
        send(below, below, 0, on_z(z + 2), recv_sem.at[0])

    @pl.when(z == 0)
    def _():
        wait_for(row, row_sem.at[top_z])
        send(row, row, 9, on_z(top_z), row_sem.at[0])
        wait_for(below, recv_sem.at[0])

    small[2].wait()
    small[3].wait()
    req = [req_ref[s] for s in range(slots)]
    length = [len_ref[s] for s in range(slots)]
    lane512 = iota((LANES, 2 * NC * LANES), 1)
    sub512 = iota((LANES, 2 * NC * LANES), 0)
    place = []
    for cc in range(NC):
        m = lane512 % LANES
        want = jnp.where((lane512 // LANES) % 2 == 0, req[0], req[1]) * width + m % width
        piece = (lane512 // (2 * LANES)) * NC + cc
        place.append(((sub512 == want) & (m // width == piece)).astype(BF16))

    for i in range(3, NZ):

        @pl.when((z > 0) & (z + i < NZ))
        def _(i=i):
            wait_for(row, row_sem.at[z + i])

    @pl.when((z > 0) & (z != top_z - 1))
    def _():
        wait_for(row, row_sem.at[0])

    @pl.when((z >= top_z - 3) & (z < top_z - 1))
    def _():
        pl.semaphore_wait(top_sem, xc)
        pl.semaphore_signal(x_sem, 1, device_id=on_z(z + 2), device_id_type=MESH)

    z_of = iota((NZ, 2 * LANES), 0)
    z_of = 2 * (z_of % G) + z_of // G
    from_below = (z_of > 0) & (z_of < jnp.where(z == 0, top_z, z))
    rows = jnp.where(from_below, below[:, 0, :], above[:, 0, :]).astype(BF16)
    row1 = c * NX + x
    g2[pl.ds(row1, 1)] = rows[:, 0:LANES][None]
    kv2[pl.ds(row1, 1)] = rows[:, LANES : 2 * LANES][None]

    pl.semaphore_wait(x_sem, 1)
    for dx, dc in others:
        send(g2.at[row1], g2.at[row1], 1, plane_mate(dx, dc, z))
    pl.semaphore_signal(pair_sem, 1, device_id=at(x, 2 * zh + 1 - zl, c), device_id_type=MESH)
    for load in loads:
        load.wait()
    wait_for(g2.at[pl.ds(0, xc - 1)], recv_sem.at[1])

    picked = [None, None]
    for cc in range(NC):
        lhs = g2[cc * NX : (cc + 1) * NX].reshape(NX * NZ, LANES)
        placed = jnp.dot(lhs, place[cc], preferred_element_type=F32).reshape(NX, NZ, 4 * LANES)
        for s in range(slots):
            for zp in range(2):
                at_lane = (zp * 2 + s) * LANES
                part = placed[:, zp * G : (zp + 1) * G, at_lane : at_lane + LANES]
                picked[s] = part if picked[s] is None else picked[s] + part
    for s in range(slots):
        qscr[s] = picked[s].astype(BF16)
    pl.semaphore_wait(pair_sem, 1)

    lane = iota((G, LANES), 1)
    lane_s, lane_hh, lane_r = (lane // 8) % 2, (lane // 4) % 2, lane % 4
    inside = [iota((G, block), 1) < length[s] for s in range(slots)]
    order = FAR_X + (0,)
    weights, vals = {}, {}
    numbered = list(enumerate(order))
    for part in (numbered[0:3], numbered[3:]):
        for n, dx in part:
            k = (x + dx) % NX
            cols = pl.ds(pl.multiple_of(k * DH, DH), DH)
            tops, sums = [], []
            for s in range(slots):
                qk = qscr[s, k]
                sc = lax.dot_general(
                    qk, kbuf[s, :, cols], (((1,), (1,)), ((), ())), preferred_element_type=F32
                )
                sc = jnp.where(inside[s], sc * scale, NEG)
                top = jnp.max(sc, axis=1, keepdims=True)
                w = jnp.exp(sc - top)
                tops.append(top)
                sums.append(jnp.sum(w, axis=1, keepdims=True))
                weights[n, s] = w.astype(BF16)
            of_slot = [
                jnp.where(
                    lane < 64,
                    jnp.where(lane_r == req[s], tops[s], NEG),
                    jnp.where(lane_r == req[s], sums[s], 0.0),
                )
                for s in range(slots)
            ]
            vals[n] = jnp.where(lane_s == 0, of_slot[0], of_slot[1])
        for n, dx in part:
            k = (x + dx) % NX
            cols = pl.ds(pl.multiple_of(k * DH, DH), DH)
            for d in range(4):
                sml[n, d] = jnp.where(
                    lane_hh[0:1] == 0, vals[n][2 * d : 2 * d + 1], vals[n][2 * d + 1 : 2 * d + 2]
                )
            o = [
                jnp.dot(weights[n, s], vbuf[s, :, cols], preferred_element_type=F32)
                for s in range(slots)
            ]
            for d in range(4):
                four = jnp.concatenate([o[s][2 * d : 2 * d + 2] for s in range(slots)], axis=0)
                so[n, d] = four.astype(BF16)
            for dd in range(4):
                if dx or dd:
                    d = dd if dx else (mine_d + dd) % 4
                    there = at(k, 2 * zh + d % 2, d // 2)
                    send(sml.at[n, d], rml.at[mine], 4, there)
                    send(so.at[n, d], ro.at[mine], 3, there)
    last = len(order) - 1
    ro[pl.ds(mine, 1)] = so[last, pl.ds(mine_d, 1)]
    rml[pl.ds(mine, 1)] = sml[last, pl.ds(mine_d, 1)]

    for dx, dc in others:
        send(kv2.at[row1], kv2.at[row1], 2, plane_mate(dx, dc, z))

    group = 4 * NX
    wait_for(rml.at[pl.ds(0, group - 1)], recv_sem.at[4])
    ml = rml[:, 0, :]
    top = jnp.max(ml, axis=0, keepdims=True)
    top = jnp.maximum(top, pltpu.roll(top, 8, 1))
    w = jnp.exp(ml - top)
    total = jnp.sum(w * pltpu.roll(ml, 64, 1), axis=0, keepdims=True)
    total = total + pltpu.roll(total, 8, 1)
    lane1 = iota((1, LANES), 1)
    aml[pl.ds(z, 1)] = jnp.where(lane1 < 64, top, pltpu.roll(total, 64, 1))[None]
    wait_for(ro.at[pl.ds(0, group - 1)], recv_sem.at[3])
    got[...] = ro[...].astype(F32)
    merged = []
    for hh in range(2):
        planes = [got[:, s * 2 + hh, :] for s in range(slots)]
        for r in range(requests):
            acc = None
            for s in range(slots):
                i = 16 + s * 8 + hh * 4 + r
                part = w[:, i : i + 1] * planes[s]
                acc = part if acc is None else acc + part
            merged.append(jnp.sum(acc, axis=0, keepdims=True))
    ao[pl.ds(z, 1)] = jnp.concatenate(merged, axis=0).astype(BF16)[None]

    for i in range(NZ):

        @pl.when(z != i)
        def _(i=i):
            send(aml.at[z], aml.at[z], 6, on_z(i))
            send(ao.at[z], ao.at[z], 5, on_z(i))

    wait_for(kv2.at[pl.ds(0, xc - 1)], recv_sem.at[2])
    total_rows = NZ * xc
    u, col = iota((2 * xc, total_rows), 0), iota((2 * xc, total_rows), 1)
    zi = (u % xc) // NC
    from_row = (u % NC) * NX + x // 2 + (NX // 2) * (u // xc)
    source = from_row * NZ + (zi % 2) * G + (x % 2) * (G // 2) + zi // 2
    pick = (col == source).astype(BF16)
    new = jnp.dot(pick, kv2[...].reshape(total_rows, LANES), preferred_element_type=F32)
    wide_l, wide_m = iota((LANES, requests * LANES), 0), iota((LANES, requests * LANES), 1)
    wide_r, wide_m = wide_m // LANES, wide_m % LANES
    to_new = (wide_l == wide_r * new_width + wide_m % new_width).astype(BF16)
    to_q = (wide_l == wide_r * width + wide_m % width).astype(BF16)
    new = jnp.dot(new.astype(BF16), to_new, preferred_element_type=F32)
    keep = (iota(new.shape, 1) % LANES) // new_width == iota(new.shape, 0) % xc
    new = jnp.where(keep, new, 0.0)

    def by_request(flat):
        return [flat[:, r * LANES : (r + 1) * LANES] for r in range(requests)]

    new_k = by_request(jnp.sum(new[0:xc], axis=0, keepdims=True))
    new_v = by_request(jnp.sum(new[xc : 2 * xc], axis=0, keepdims=True))
    u, col = iota((16, total_rows), 0), iota((16, total_rows), 1)
    source = ((u % NC) * NX + x) * NZ + ((u % 4) // NC) * G + 4 * c + u // 4
    pick = (col == source).astype(BF16)
    own_q = jnp.dot(pick, g2[...].reshape(total_rows, LANES), preferred_element_type=F32)
    own_q = jnp.dot(own_q.astype(BF16), to_q, preferred_element_type=F32)
    keep = (iota(own_q.shape, 1) % LANES) // width == iota(own_q.shape, 0) % 4
    own_q = jnp.where(keep, own_q, 0.0)
    k_rows = jnp.concatenate(new_k + new_k, axis=0)
    v_rows = jnp.concatenate(new_v + new_v, axis=0)
    new_score = []
    for half in range(2):
        q_rows = []
        for hh in range(2):
            i = (half * 2 + hh) * 4
            q_rows += by_request(jnp.sum(own_q[i : i + 4], axis=0, keepdims=True))
        q_rows = jnp.concatenate(q_rows, axis=0)
        new_score.append(jnp.sum(q_rows * k_rows, axis=1, keepdims=True) * scale)

    wait_for(aml.at[pl.ds(0, NZ - 1)], recv_sem.at[6])
    sub = iota((8, LANES), 0)
    lane8 = iota((8, LANES), 1)
    m_at, l_at = lane8 == 16 + sub, lane8 == 80 + sub
    ways = []
    for half in range(2):
        planes = range(half, NZ, 2)
        ms = [jnp.sum(jnp.where(m_at, aml[i], 0.0), axis=1, keepdims=True) for i in planes]
        ls = [jnp.sum(jnp.where(l_at, aml[i], 0.0), axis=1, keepdims=True) for i in planes]
        peak = functools.reduce(jnp.maximum, ms, new_score[half])
        new_w = jnp.exp(new_score[half] - peak)
        factors = [jnp.exp(m - peak) for m in ms]
        denom = new_w
        for factor, part in zip(factors, ls):
            denom = denom + factor * part
        ways.append((new_w, factors, denom))
    wait_for(ao.at[pl.ds(0, NZ - 1)], recv_sem.at[5])
    base = pl.multiple_of((x * NC + c) * 4 * DH, 4 * DH)
    for half in range(2):
        new_w, factors, denom = ways[half]
        numer = new_w * v_rows
        for i, factor in zip(range(half, NZ, 2), factors):
            numer = numer + factor * ao[i].astype(F32)
        final = (numer / denom).astype(BF16)
        for hh in range(2):
            start = pl.multiple_of(base + (half * 2 + hh) * DH, DH)
            out_ref[:, pl.ds(start, DH)] = final[hh * 4 : hh * 4 + 4]

    here = out_ref.at[:, pl.ds(base, 4 * DH)]
    for dx, dc in others:
        send(here, here, 7, plane_mate(dx, dc, z))
    wait_for(out_ref.at[:, pl.ds(0, (xc - 1) * 4 * DH)], recv_sem.at[7])

    for i in range(1, NZ):

        @pl.when(greeter(i) if i > 1 else z != 1)
        def _(i=i):
            wait_for(row, send_sem.at[8 + i])

    @pl.when((z > 0) & (z < top_z))
    def _():
        wait_for(row, send_sem.at[8 + NZ])

    @pl.when((z > 0) & (z < top_z - 1))
    def _():
        wait_for(below, send_sem.at[0])

    @pl.when(z == top_z - 1)
    def _():
        wait_for(below, send_sem.at[8])

    wait_for(g2.at[pl.ds(0, xc - 1)], send_sem.at[1])
    wait_for(kv2.at[pl.ds(0, xc - 1)], send_sem.at[2])
    wait_for(ro.at[pl.ds(0, group - 1)], send_sem.at[3])
    wait_for(rml.at[pl.ds(0, group - 1)], send_sem.at[4])
    wait_for(ao.at[pl.ds(0, NZ - 1)], send_sem.at[5])
    wait_for(aml.at[pl.ds(0, NZ - 1)], send_sem.at[6])
    wait_for(out_ref.at[:, pl.ds(0, (xc - 1) * 4 * DH)], send_sem.at[7])


def shards(queries, new_kv, keys, values, slot_request, slot_length):
    slots, block, columns = keys.shape
    requests = queries.shape[0]
    xc, group = NX * NC, 4 * NX
    vmem = pl.BlockSpec(memory_space=pltpu.VMEM)
    hbm = pl.BlockSpec(memory_space=pl.ANY)
    return pl.pallas_call(
        kernel,
        out_shape=pltpu.VMEM((requests, H * DH), BF16),
        in_specs=[hbm] * 6,
        out_specs=vmem,
        scratch_shapes=[
            pltpu.SMEM(slot_request.shape, jnp.int32),
            pltpu.SMEM(slot_length.shape, jnp.int32),
            pltpu.VMEM(queries.shape, BF16),
            pltpu.VMEM(new_kv.shape, BF16),
            pltpu.VMEM((slots, block, columns), BF16),
            pltpu.VMEM((slots, block, columns), BF16),
            pltpu.VMEM((NZ, 1, 2 * LANES), F32),
            pltpu.VMEM((NZ, 1, 2 * LANES), F32),
            pltpu.VMEM((xc, NZ, LANES), BF16),
            pltpu.VMEM((xc, NZ, LANES), BF16),
            pltpu.VMEM((slots, KVH, G, DH), BF16),
            pltpu.VMEM((KVH, 4, 4, DH), BF16),
            pltpu.VMEM((KVH, 4, 1, LANES), F32),
            pltpu.VMEM((group, 4, DH), BF16),
            pltpu.VMEM((group, 4, DH), F32),
            pltpu.VMEM((group, 1, LANES), F32),
            pltpu.VMEM((NZ, 8, DH), BF16),
            pltpu.VMEM((NZ, 1, LANES), F32),
            pltpu.SemaphoreType.DMA((2 * slots,)),
            pltpu.SemaphoreType.DMA((4,)),
            pltpu.SemaphoreType.DMA((9 + NZ,)),
            pltpu.SemaphoreType.DMA((8,)),
            pltpu.SemaphoreType.DMA((NZ,)),
            pltpu.SemaphoreType.REGULAR,
            pltpu.SemaphoreType.REGULAR,
            pltpu.SemaphoreType.REGULAR,
        ],
        compiler_params=pltpu.CompilerParams(collective_id=0, has_side_effects=True),
        cost_estimate=pl.CostEstimate(
            flops=4 * slots * block * H * DH,
            bytes_accessed=4 * slots * block * columns,
            transcendentals=slots * block * H,
        ),
        name="decode",
    )(slot_request, slot_length, queries, new_kv, keys, values)


def solution(mesh):
    torus = Mesh(mesh.devices.reshape(mesh.shape["parts"], NX, NZ, NC), ("parts",) + SEQ)
    placed = (
        P("parts", SEQ),
        P("parts", SEQ),
        P(PARTS_SEQ, None, None),
        P(PARTS_SEQ, None, None),
        P(PARTS_SEQ),
        P(PARTS_SEQ),
    )
    return jax.shard_map(
        shards, mesh=torus, in_specs=placed, out_specs=P("parts", None), check_vma=False
    )
```
